32 devices in a mesh: inl: 4 (over z), xln: 8 (over y, x, core).
Axes of the slice: x: 2, y: 2, z: 4, core: 2. Of those that a mesh axis runs over, the one named last changes fastest.
Arguments:
- noisy: float32 [128, 256, 512], P('inl', 'xln'), may hold values from -6 to 6
- bound: float32 [128, 256, 512], P('inl', 'xln'), may hold values from 0.05 to 0.5
Outputs:
- denoised: float32 [128, 256, 512], P('inl', 'xln')
- dual: float32 [3, 128, 256, 512], P(None, 'inl', 'xln')
- norms: float32 [2, 2], replicated
The draws below stay inside these ranges and needn't reach their ends.
All inputs are finite; a program needn't handle non-finite values.
Results may differ from the reference program's by a relative error of at most 0.0001.
Values sent between devices are 32-bit elements; how exact they have to be, the bound alone decides.
A program may use at most 64 MiB of HBM per device.

```python
import math
import jax
import jax.numpy as jnp
from jax import lax

NZ = 512
ITERS = 2
NI = 128
NX = 256


def levels(key, shape, cuts, least, high):
    def one(position, blocks):
        draws = jax.random.uniform(jax.random.fold_in(jax.random.fold_in(key, 6), position), (blocks,), jnp.float32, least / len(cuts), high / len(cuts))
        return jnp.repeat(jnp.exp(draws), shape[position] // blocks).reshape((-1,) + (1,) * (len(shape) - position - 1))

    gain = one(*cuts[0])
    for cut in cuts[1:]:
        gain = gain * one(*cut)
    return gain


def bell_draw(stream_key, extent, spread, most, split=(), held_as=jnp.bfloat16):
    gain = levels(stream_key, extent, split, -0.22, 0.18) if split else 1.0
    values = jax.random.normal(stream_key, extent, jnp.float32) * spread * gain
    return jnp.minimum(jnp.maximum(values, -most), most).astype(held_as)


def setup_inputs(seed: int = 0) -> dict:
    splits = jax.random.split(jax.random.key(seed), 3)
    return {
        "noisy": bell_draw(splits[0], (NI, NX, NZ), 1.0, 6.0, ((0, 4), (1, 8)), jnp.float32),
        "bound": jnp.clip(jnp.exp(math.log(0.5) - 2.3025851 * jax.random.uniform(splits[1], (NI, NX, NZ), jnp.float32) ** levels(splits[1], (NI, NX, NZ), ((0, 4), (1, 8)), -0.2, 0.2)), 0.05, 0.5),
    }


SIGMA = 0.28
TAU = 0.28

def forward(field, axis):
    first = lax.slice_in_dim(field, 0, 1, axis=axis)
    return jnp.concatenate([jnp.diff(field, axis=axis), jnp.zeros_like(first)], axis=axis)

def backward(field, axis):
    size = field.shape[axis]
    first = lax.slice_in_dim(field, 0, 1, axis=axis)
    earlier = jnp.concatenate([jnp.zeros_like(first), lax.slice_in_dim(field, 0, size - 1, axis=axis)], axis=axis)
    return field - earlier

def reference(noisy, bound):
    primal = noisy
    smooth = noisy
    dual_parts = [jnp.zeros_like(noisy) for axis in range(3)]
    rows = []
    for step in range(ITERS):
        fresh = [jnp.clip(dual_parts[axis] + SIGMA * forward(smooth, axis), -bound, bound) for axis in range(3)]
        diverge = backward(fresh[0], 0) + backward(fresh[1], 1) + backward(fresh[2], 2)
        updated = (primal + TAU * diverge + TAU * noisy) / (1.0 + TAU)
        primal_sum = jnp.sum((updated - primal) ** 2)
        dual_sum = jnp.sum((fresh[0] - dual_parts[0]) ** 2) + jnp.sum((fresh[1] - dual_parts[1]) ** 2) + jnp.sum((fresh[2] - dual_parts[2]) ** 2)
        rows.append(jnp.sqrt(jnp.stack([primal_sum, dual_sum])))
        smooth = 2.0 * updated - primal
        primal = updated
        dual_parts = fresh
    return (primal, jnp.stack(dual_parts), jnp.stack(rows))
```

```python
import functools

import jax
import jax.numpy as jnp
from jax import lax
from jax.experimental import pallas as pl
from jax.experimental.pallas import tpu as pltpu
from jax.sharding import PartitionSpec as P

SIGMA = 0.28
TAU = 0.28
GAIN = TAU / (1.0 + TAU)


def clip(value, limit):
    return jnp.minimum(jnp.maximum(value, -limit), limit)


def fold(square):
    rows, lanes = square.shape
    total = square[0:8]
    for at in range(8, rows, 8):
        total = total + square[at : at + 8]
    part = total[:, 0:128]
    for at in range(128, lanes, 128):
        part = part + total[:, at : at + 128]
    return part


def gather_lanes(rows):
    lane = lax.broadcasted_iota(jnp.int32, (1, 128), 1)
    result = jnp.zeros((1, 128), jnp.float32)
    for k, row in enumerate(rows):
        result = jnp.where(lane == k, jnp.sum(row, axis=1, keepdims=True), result)
    return result


def one_stage(ni_dev, nx_dev):
    return ni_dev <= 4 and ni_dev * nx_dev <= 32


def reduction(ni_dev, nx_dev):
    everyone = [(di, dx) for di in range(ni_dev) for dx in range(nx_dev) if di or dx]
    if one_stage(ni_dev, nx_dev):
        return [everyone]
    return [[peer for peer in everyone if peer[0] == 0], [peer for peer in everyone if peer[1] == 0]]


def stepped(start, stop, body, carry, unroll=4):
    def group(k, carry):
        for at in range(unroll):
            carry = body(start + k * unroll + at, carry)
        return carry

    whole = (stop - start) // unroll
    carry = lax.fori_loop(0, whole, group, carry)
    for i in range(start + whole * unroll, stop):
        carry = body(i, carry)
    return carry


def split(value, dim, size):
    return [lax.slice_in_dim(value, at, at + size, axis=dim) for at in range(0, value.shape[dim], size)]


def ahead(value, dim):
    size = (8, 128)[dim]
    parts = split(value, dim, size)
    turned = [pltpu.roll(part, size - 1, dim) for part in parts]
    edge = lax.broadcasted_iota(jnp.int32, parts[0].shape, dim) == size - 1
    after = turned[1:] + [parts[-1]]
    return jnp.concatenate([jnp.where(edge, a, t) for a, t in zip(after, turned)], axis=dim)


def behind(value, dim):
    size = (8, 128)[dim]
    turned = [pltpu.roll(part, 1, dim) for part in split(value, dim, size)]
    edge = lax.broadcasted_iota(jnp.int32, turned[0].shape, dim) == 0
    before = [jnp.zeros_like(turned[0])] + turned[:-1]
    return jnp.concatenate([jnp.where(edge, a, t) for a, t in zip(before, turned)], axis=dim)


def kernel(
    ni_dev, nx_dev,
    noisy, bound, out, dual, norms,
    n, b, v, step,
    nx_first, nx_last, bx_last, nx_next, nx_prev, bx_prev,
    vx_first, vx_last, vx_next, vx_prev, dx_prev, dx_edge, di_prev,
    mine, others,
    load_sem, send_sem, recv_sem, give_sem, take_sem,
):
    ni, nx, nz = noisy.shape
    top, end = ni, ni + 1
    my_i, my_x = lax.axis_index("inl"), lax.axis_index("xln")

    loads = []

    def load(src, dst):
        copy = pltpu.make_async_copy(src, dst, load_sem.at[len(loads)])
        copy.start()
        loads.append(copy)

    load(noisy.at[pl.ds(ni - 1, 1)], n.at[pl.ds(top, 1)])
    load(bound.at[pl.ds(ni - 1, 1)], b.at[pl.ds(top, 1)])
    load(noisy.at[pl.ds(0, 1)], n.at[pl.ds(1, 1)])
    load(noisy.at[pl.ds(1, ni - 2)], n.at[pl.ds(2, ni - 2)])
    load(bound.at[pl.ds(0, ni - 1)], b.at[pl.ds(1, ni - 1)])

    barrier = pltpu.get_barrier_semaphore()
    stages = reduction(ni_dev, nx_dev)

    def at(di, dx):
        return {"inl": lax.rem(my_i + di, ni_dev), "xln": lax.rem(my_x + dx, nx_dev)}

    greeted = 0
    for di in range(1 - ni_dev, ni_dev):
        for dx in range(nx_dev):
            if (di == 0 and dx == 0) or not (abs(di) <= 1 and (one_stage(ni_dev, nx_dev) or di * dx == 0) or (dx == 0 and not one_stage(ni_dev, nx_dev))):
                continue
            exists = jnp.logical_and(my_i + di >= 0, my_i + di < ni_dev)
            greeted = greeted + exists.astype(jnp.int32)

            @pl.when(exists)
            def _():
                pl.semaphore_signal(
                    barrier, inc=1,
                    device_id={"inl": my_i + di, "xln": lax.rem(my_x + dx, nx_dev)},
                    device_id_type=pl.DeviceIdType.MESH,
                )
    pl.semaphore_wait(barrier, greeted)

    sent = []

    def send(slot, src, dst, axis, forward):
        me, count = (my_i, ni_dev) if axis == "inl" else (my_x, nx_dev)
        target = lax.rem(me + (1 if forward else count - 1), count)
        copy = pltpu.make_async_remote_copy(
            src_ref=src, dst_ref=dst, send_sem=send_sem.at[slot], recv_sem=recv_sem.at[slot],
            device_id={axis: target}, device_id_type=pl.DeviceIdType.MESH,
        )
        not_last, not_first = me < count - 1, me > 0
        can_send, can_recv = (not_last, not_first) if forward else (not_first, not_last)

        @pl.when(can_send)
        def _():
            copy.start()

        sent.append((copy, can_send))

        def arrive(fill):
            @pl.when(can_recv)
            def _():
                copy.wait_recv()

            @pl.when(jnp.logical_not(can_recv))
            def _():
                fill()

        return arrive

    def setter(dst, src):
        def fill():
            dst[...] = src[...]

        return fill

    loads[0].wait()
    got_n_prev = send(0, n.at[top], n.at[0], "inl", True)
    loads[1].wait()
    got_b_prev = send(1, b.at[top], b.at[0], "inl", True)
    loads[2].wait()
    got_n_next = send(2, n.at[1], n.at[end], "inl", False)
    loads[3].wait()
    nx_last[...] = n[1:end, nx - 1, :]
    got_nx_prev = send(3, nx_last, nx_prev, "xln", True)
    nx_first[...] = n[1:end, 0, :]
    got_nx_next = send(5, nx_first, nx_next, "xln", False)
    loads[4].wait()
    bx_last[...] = b[1:end, nx - 1, :]
    got_bx_prev = send(4, bx_last, bx_prev, "xln", True)

    step[...] = jnp.zeros_like(step)

    def squares(oi, ox, oz):
        return fold(oi * oi + ox * ox + oz * oz)

    def pass_one(i, d1):
        here, limit = n[i + 1], b[i + 1]
        di = clip(SIGMA * (n[i + 2] - here), limit)
        dx = clip(SIGMA * (ahead(here, 0) - here), limit)
        dz = clip(SIGMA * (ahead(here, 1) - here), limit)
        dual[0, i] = di
        dual[1, i] = dx
        dual[2, i] = dz
        div = di - step[...]
        div = div + (dx - behind(dx, 0))
        div = div + (dz - behind(dz, 1))
        step[...] = di
        v[i + 1] = here + (2.0 * GAIN) * div
        return d1 + squares(di, dx, dz)

    zero = jnp.zeros((8, 128), jnp.float32)
    d1 = stepped(0, ni - 1, pass_one, zero)
    here, limit = n[top], b[top]
    dx = clip(SIGMA * (ahead(here, 0) - here), limit)
    dz = clip(SIGMA * (ahead(here, 1) - here), limit)
    dual[1, ni - 1] = dx
    dual[2, ni - 1] = dz
    div = (dx - behind(dx, 0)) - step[...]
    div = div + (dz - behind(dz, 1))
    v[top] = here + (2.0 * GAIN) * div
    d1 = d1 + fold(dx * dx + dz * dz)

    got_nx_prev(setter(nx_prev, nx_first))
    got_bx_prev(setter(bx_prev, bx_last))
    got_nx_next(setter(nx_next, nx_last))
    dx_last = clip(SIGMA * (nx_next[...] - nx_last[...]), bx_last[...])
    dxp = clip(SIGMA * (nx_first[...] - nx_prev[...]), bx_prev[...])
    dual[1, :, nx - 1, :] = dx_last
    dx_prev[...] = dxp
    dx_edge[...] = dx_last
    v[1:end, nx - 1, :] = v[1:end, nx - 1, :] + (2.0 * GAIN) * dx_last
    v[1:end, 0, :] = v[1:end, 0, :] - (2.0 * GAIN) * dxp

    got_n_prev(setter(n.at[0], n.at[1]))
    got_b_prev(setter(b.at[0], b.at[1]))
    got_n_next(setter(n.at[end], n.at[top]))
    di_last = clip(SIGMA * (n[end] - n[top]), b[top])
    dip = clip(SIGMA * (n[1] - n[0]), b[0])
    dual[0, ni - 1] = di_last
    di_prev[...] = dip
    v[top] = v[top] + (2.0 * GAIN) * di_last
    v[1] = v[1] - (2.0 * GAIN) * dip
    got_v_prev = send(6, v.at[top], v.at[0], "inl", True)
    got_v_next = send(7, v.at[1], v.at[end], "inl", False)
    vx_last[...] = v[1:end, nx - 1, :]
    got_vx_prev = send(8, vx_last, vx_prev, "xln", True)
    vx_first[...] = v[1:end, 0, :]
    got_vx_next = send(9, vx_first, vx_next, "xln", False)
    d1 = d1 + fold(di_last * di_last) + fold(dx_last * dx_last)

    row = lax.broadcasted_iota(jnp.int32, (8, nz), 0)

    def inner_rows(value):
        parts = split(value, 0, 8)
        parts[0] = jnp.where(row == 0, 0.0, parts[0])
        parts[-1] = jnp.where(row == 7, 0.0, parts[-1])
        return jnp.concatenate(parts, axis=0)

    def pass_two(i, sums):
        p1, p2, d2 = sums
        here, limit, base = v[i + 1], b[i + 1], n[i + 1]
        oi, ox, oz = dual[0, i], dual[1, i], dual[2, i]
        di = clip(oi + SIGMA * (v[i + 2] - here), limit)
        dx = clip(ox + SIGMA * (ahead(here, 0) - here), limit)
        dz = clip(oz + SIGMA * (ahead(here, 1) - here), limit)
        dual[0, i] = di
        dual[1, i] = dx
        dual[2, i] = dz
        div = di - step[...]
        div = div + (dx - behind(dx, 0))
        div = div + (dz - behind(dz, 1))
        step[...] = di
        half = 0.5 * (here - base)
        change = GAIN * (div - half)
        out[i] = base + half + change
        inner = inner_rows(change)
        return (
            p1 + fold(half * half),
            p2 + fold(inner * inner),
            d2 + squares(di - oi, dx - ox, dz - oz),
        )

    step[...] = clip(dual[0, 0] + SIGMA * (v[2] - v[1]), b[1])
    sums = stepped(1, ni - 1, pass_two, (zero,) * 3)

    got_v_next(setter(v.at[end], v.at[top]))
    sums = pass_two(ni - 1, sums)
    got_v_prev(setter(v.at[0], v.at[1]))
    step[...] = clip(di_prev[...] + SIGMA * (v[1] - v[0]), b[0])
    p1, p2, d2 = pass_two(0, sums)

    got_vx_prev(setter(vx_prev, vx_first))
    got_vx_next(setter(vx_next, vx_last))
    was = dx_edge[...]
    dx_last = clip(was + SIGMA * (vx_next[...] - vx_last[...]), bx_last[...])
    dual[1, :, nx - 1, :] = dx_last
    moved = dx_last - was
    d2 = d2 + fold(moved * moved)
    u_last = out[:, nx - 1, :] + GAIN * moved
    out[:, nx - 1, :] = u_last
    dxp = clip(dx_prev[...] + SIGMA * (vx_first[...] - vx_prev[...]), bx_prev[...])
    u_first = out[:, 0, :] - GAIN * dxp
    out[:, 0, :] = u_first
    change = u_last - (nx_last[...] + 0.5 * (vx_last[...] - nx_last[...]))
    p2 = p2 + fold(change * change)
    change = u_first - (nx_first[...] + 0.5 * (vx_first[...] - nx_first[...]))
    p2 = p2 + fold(change * change)

    total = gather_lanes([jnp.sum(part, axis=0, keepdims=True) for part in (p1, d1, p2, d2)])
    copies = []
    for stage, peers in enumerate(stages):
        mine[stage] = total
        first = len(copies)
        for k, (di, dx) in enumerate(peers, first):
            copy = pltpu.make_async_remote_copy(
                src_ref=mine.at[stage], dst_ref=others.at[k],
                send_sem=give_sem.at[k], recv_sem=take_sem.at[k],
                device_id=at(di, dx), device_id_type=pl.DeviceIdType.MESH,
            )
            copy.start()
            copies.append(copy)
        for k in range(first, len(copies)):
            copies[k].wait_recv()
            total = total + others[k]
    norms[...] = jnp.sqrt(jnp.concatenate([total, pltpu.roll(total, 126, 1)], axis=0)[:, 0:2])

    for copy in copies:
        copy.wait_send()
    for copy, can_send in sent:
        @pl.when(can_send)
        def _():
            copy.wait_send()


def put_out(out_held, dual_held, norms_held, out, dual, norms, sems):
    half = out.shape[0] // 2
    pairs = [(norms_held, norms)]
    for at in (0, half):
        part = pl.ds(at, half)
        pairs.append((out_held.at[part], out.at[part]))
        for axis in range(3):
            pairs.append((dual_held.at[axis, part], dual.at[axis, part]))
    copies = [pltpu.make_async_copy(src, dst, sems.at[k]) for k, (src, dst) in enumerate(pairs)]
    for copy in copies:
        copy.start()
    for copy in copies:
        copy.wait()


def per_device(noisy, bound):
    ni, nx, nz = noisy.shape
    ni_dev, nx_dev = lax.axis_size("inl"), lax.axis_size("xln")
    f32 = jnp.float32
    face = pltpu.VMEM((ni, nz), f32)
    slab = pltpu.VMEM((nx, nz), f32)
    dma = pltpu.SemaphoreType.DMA
    volume = 4 * ni * nx * nz
    stages = reduction(ni_dev, nx_dev)
    peers = sum(len(stage) for stage in stages)
    noisy = pltpu.with_memory_space_constraint(noisy, pltpu.HBM)
    bound = pltpu.with_memory_space_constraint(bound, pltpu.HBM)
    held = pl.pallas_call(
        functools.partial(kernel, ni_dev, nx_dev),
        out_shape=(
            pltpu.VMEM((ni, nx, nz), f32),
            pltpu.VMEM((3, ni, nx, nz), f32),
            pltpu.VMEM((2, 2), f32),
        ),
        in_specs=[pl.BlockSpec(memory_space=pltpu.HBM)] * 2,
        out_specs=(
            pl.BlockSpec(memory_space=pltpu.VMEM),
            pl.BlockSpec(memory_space=pltpu.VMEM),
            pl.BlockSpec(memory_space=pltpu.VMEM),
        ),
        scratch_shapes=[
            pltpu.VMEM((ni + 2, nx, nz), f32),
            pltpu.VMEM((ni + 1, nx, nz), f32),
            pltpu.VMEM((ni + 2, nx, nz), f32),
            slab,
            *([face] * 12),
            slab,
            pltpu.VMEM((len(stages), 1, 128), f32),
            pltpu.VMEM((peers, 1, 128), f32),
            dma((5,)), dma((10,)), dma((10,)), dma((peers,)), dma((peers,)),
        ],
        compiler_params=pltpu.CompilerParams(
            collective_id=0, has_side_effects=True, vmem_limit_bytes=24 * 1024 * 1024
        ),
        cost_estimate=pl.CostEstimate(
            flops=80 * ni * nx * nz, bytes_accessed=6 * volume, transcendentals=0
        ),
        name="denoise",
    )(noisy, bound)
    in_vmem = pl.BlockSpec(memory_space=pltpu.VMEM)
    in_hbm = pl.BlockSpec(memory_space=pltpu.HBM)
    return pl.pallas_call(
        put_out,
        out_shape=(
            jax.ShapeDtypeStruct((ni, nx, nz), f32),
            jax.ShapeDtypeStruct((3, ni, nx, nz), f32),
            jax.ShapeDtypeStruct((2, 2), f32),
        ),
        in_specs=[in_vmem] * 3,
        out_specs=(in_hbm,) * 3,
        scratch_shapes=[dma((9,))],
        compiler_params=pltpu.CompilerParams(vmem_limit_bytes=1024 * 1024),
        cost_estimate=pl.CostEstimate(flops=0, bytes_accessed=4 * volume, transcendentals=0),
        name="put_out",
    )(*held)


def solution(mesh):
    in_specs = (P("inl", "xln", None), P("inl", "xln", None))
    out_specs = (P("inl", "xln", None), P(None, "inl", "xln", None), P())
    return jax.shard_map(
        per_device, mesh=mesh, in_specs=in_specs, out_specs=out_specs, check_vma=False
    )
```

```python
import functools

import jax
import jax.numpy as jnp
from jax import lax
from jax.experimental import pallas as pl
from jax.experimental.pallas import tpu as pltpu
from jax.sharding import PartitionSpec as P

SIGMA = 0.28
TAU = 0.28
GAIN = TAU / (1.0 + TAU)
GROUP = 4
MIDDLE = 7
RIM = 7


def clip(value, limit):
    return jnp.minimum(jnp.maximum(value, -limit), limit)


def fold(square):
    rows, lanes = square.shape
    total = square[0:8]
    for at in range(8, rows, 8):
        total = total + square[at : at + 8]
    part = total[:, 0:128]
    for at in range(128, lanes, 128):
        part = part + total[:, at : at + 128]
    return part


def gather_lanes(rows):
    lane = lax.broadcasted_iota(jnp.int32, (1, 128), 1)
    result = jnp.zeros((1, 128), jnp.float32)
    for k, row in enumerate(rows):
        result = jnp.where(lane == k, jnp.sum(row, axis=1, keepdims=True), result)
    return result


def one_stage(ni_dev, nx_dev):
    return ni_dev <= 4 and ni_dev * nx_dev <= 32


def reduction(ni_dev, nx_dev):
    everyone = [(di, dx) for di in range(ni_dev) for dx in range(nx_dev) if di or dx]
    if one_stage(ni_dev, nx_dev):
        return [everyone]
    return [[peer for peer in everyone if peer[0] == 0], [peer for peer in everyone if peer[1] == 0]]


def stepped(start, stop, body, carry, unroll=4):
    def group(k, carry):
        for at in range(unroll):
            carry = body(start + k * unroll + at, carry)
        return carry

    whole = (stop - start) // unroll
    carry = lax.fori_loop(0, whole, group, carry)
    for i in range(start + whole * unroll, stop):
        carry = body(i, carry)
    return carry


def split(value, dim, size):
    return [lax.slice_in_dim(value, at, at + size, axis=dim) for at in range(0, value.shape[dim], size)]


def ahead(value, dim):
    size = (8, 128)[dim]
    parts = split(value, dim, size)
    turned = [pltpu.roll(part, size - 1, dim) for part in parts]
    edge = lax.broadcasted_iota(jnp.int32, parts[0].shape, dim) == size - 1
    after = turned[1:] + [parts[-1]]
    return jnp.concatenate([jnp.where(edge, a, t) for a, t in zip(after, turned)], axis=dim)


def behind(value, dim):
    size = (8, 128)[dim]
    turned = [pltpu.roll(part, 1, dim) for part in split(value, dim, size)]
    edge = lax.broadcasted_iota(jnp.int32, turned[0].shape, dim) == 0
    before = [jnp.zeros_like(turned[0])] + turned[:-1]
    return jnp.concatenate([jnp.where(edge, a, t) for a, t in zip(before, turned)], axis=dim)


def kernel(
    ni_dev, nx_dev,
    noisy, bound, out, dual, norms,
    n, b, v, step,
    nx_first, nx_last, bx_last, bx_first, nx_second, nx_semi, bx_semi,
    nx_next, nx_prev, bx_prev,
    vx_first, vx_last, vx_next, vx_prev, wx_first, wx_last, dx_prev, dx_edge,
    zc_up, zc_down, zc_prev, zc_next, xc_up, xc_down, xc_prev, xc_next,
    mine, others,
    load_sem, chunk_sem, send_sem, recv_sem, give_sem, take_sem, far_sem,
):
    ni, nx, nz = noisy.shape
    top, end = ni, ni + 1
    my_i, my_x = lax.axis_index("inl"), lax.axis_index("xln")
    f32 = jnp.float32

    barrier = pltpu.get_barrier_semaphore()
    stages = reduction(ni_dev, nx_dev)

    def at(di, dx):
        return {"inl": lax.rem(my_i + di, ni_dev), "xln": lax.rem(my_x + dx, nx_dev)}

    greeted = 0
    for di in range(1 - ni_dev, ni_dev):
        for dx in range(nx_dev):
            if (di == 0 and dx == 0) or di * dx or (abs(di) > 1 and one_stage(ni_dev, nx_dev)):
                continue
            exists = jnp.logical_and(my_i + di >= 0, my_i + di < ni_dev)
            greeted = greeted + exists.astype(jnp.int32)

            @pl.when(exists)
            def _():
                pl.semaphore_signal(
                    barrier, inc=1,
                    device_id={"inl": my_i + di, "xln": lax.rem(my_x + dx, nx_dev)},
                    device_id_type=pl.DeviceIdType.MESH,
                )

    loads = []

    def load(src, dst):
        copy = pltpu.make_async_copy(src, dst, load_sem.at[len(loads)])
        copy.start()
        loads.append(copy)

    load(noisy.at[:, 0, :], nx_first)
    load(noisy.at[:, nx - 1, :], nx_last)
    load(bound.at[:, nx - 1, :], bx_last)
    load(bound.at[:, 0, :], bx_first)
    load(noisy.at[pl.ds(ni - 1, 1)], n.at[pl.ds(top, 1)])
    load(bound.at[pl.ds(ni - 1, 1)], b.at[pl.ds(top, 1)])
    load(noisy.at[pl.ds(0, 1)], n.at[pl.ds(1, 1)])
    load(noisy.at[:, 1, :], nx_second)
    load(noisy.at[:, nx - 2, :], nx_semi)
    load(bound.at[:, nx - 2, :], bx_semi)
    def chunk(k, size):
        return (
            pltpu.make_async_copy(
                noisy.at[pl.ds(GROUP * k + 1, size)], n.at[pl.ds(GROUP * k + 2, size)], chunk_sem.at[0, k]
            ),
            pltpu.make_async_copy(
                bound.at[pl.ds(GROUP * k, size)], b.at[pl.ds(GROUP * k + 1, size)], chunk_sem.at[1, k]
            ),
        )

    groups = (ni - 1) // GROUP
    rest = ni - 1 - groups * GROUP
    pieces = [(k, GROUP) for k in range(groups)]
    tail = pltpu.make_async_copy(
        bound.at[pl.ds(ni - 1 - rest, rest)], b.at[pl.ds(ni - rest, rest)], chunk_sem.at[1, groups]
    )
    tail_n = pltpu.make_async_copy(
        noisy.at[pl.ds(ni - rest, rest - 1)], n.at[pl.ds(ni - rest + 1, rest - 1)], chunk_sem.at[0, groups]
    )
    for k, size in pieces:
        for copy in chunk(k, size):
            copy.start()
    tail.start()
    tail_n.start()

    sent = []

    def send(src, dst, axis, forward):
        slot = len(sent)
        me, count = (my_i, ni_dev) if axis == "inl" else (my_x, nx_dev)
        target = lax.rem(me + (1 if forward else count - 1), count)
        copy = pltpu.make_async_remote_copy(
            src_ref=src, dst_ref=dst, send_sem=send_sem.at[slot], recv_sem=recv_sem.at[slot],
            device_id={axis: target}, device_id_type=pl.DeviceIdType.MESH,
        )
        not_last, not_first = me < count - 1, me > 0
        can_send, can_recv = (not_last, not_first) if forward else (not_first, not_last)

        @pl.when(can_send)
        def _():
            copy.start()

        sent.append((copy, can_send))

        def arrive(fill):
            @pl.when(can_recv)
            def _():
                copy.wait_recv()

            @pl.when(jnp.logical_not(can_recv))
            def _():
                fill()

        return arrive

    def left(slot):
        copy, can_send = sent[slot]

        @pl.when(can_send)
        def _():
            copy.wait_send()

    def setter(dst, src):
        def fill():
            dst[...] = src[...]

        return fill

    first, last = slice(0, 1), slice(ni - 1, ni)

    step[...] = jnp.zeros_like(step)

    def squares(oi, ox, oz):
        return fold(oi * oi + ox * ox + oz * oz)

    def pass_one(i, d1):
        here, limit = n[i + 1], b[i + 1]
        di = clip(SIGMA * (n[i + 2] - here), limit)
        dx = clip(SIGMA * (ahead(here, 0) - here), limit)
        dz = clip(SIGMA * (ahead(here, 1) - here), limit)
        dual[0, i] = di
        dual[1, i] = dx
        dual[2, i] = dz
        div = di - step[...]
        div = div + (dx - behind(dx, 0))
        div = div + (dz - behind(dz, 1))
        step[...] = di
        v[i + 1] = here + (2.0 * GAIN) * div
        return d1 + squares(di, dx, dz)

    zero = jnp.zeros((8, 128), jnp.float32)

    def pass_group(k, d1):
        for copy in chunk(k, GROUP):
            copy.wait()
        for at in range(GROUP):
            d1 = pass_one(GROUP * k + at, d1)
        return d1

    for k in range(10):
        loads[k].wait()

    def edge(here, limit, side):
        di = clip(SIGMA * (ahead(here, 0) - here), limit)
        dz = clip(SIGMA * (ahead(here, 1) - here), limit)
        return here + (2.0 * GAIN) * ((di - behind(di, 0)) + side + (dz - behind(dz, 1)))

    inward = clip(SIGMA * (nx_second[...] - nx_first[...]), bx_first[...])
    vx_first[...] = edge(nx_first[...], bx_first[...], inward)
    inward = clip(SIGMA * (nx_last[...] - nx_semi[...]), bx_semi[...])
    vx_last[...] = edge(nx_last[...], bx_last[...], -inward)

    early = 2
    d1 = lax.fori_loop(0, early, pass_group, zero)
    pl.semaphore_wait(barrier, greeted)
    zc_up[0:1], zc_up[1:2], zc_up[2:3], zc_up[3:4] = nx_first[last], nx_last[last], bx_first[last], bx_last[last]
    zc_down[0:1], zc_down[1:2] = nx_first[first], nx_last[first]
    xc_up[0:1], xc_up[1:2], xc_up[2:3], xc_up[3:4] = nx_last[first], nx_last[last], bx_last[first], bx_last[last]
    xc_down[0:1], xc_down[1:2] = nx_first[first], nx_first[last]
    got_zc_prev = send(zc_up, zc_prev, "inl", True)
    got_zc_next = send(zc_down, zc_next, "inl", False)
    got_xc_prev = send(xc_up, xc_prev, "xln", True)
    got_xc_next = send(xc_down, xc_next, "xln", False)
    got_nx_prev = send(nx_last, nx_prev, "xln", True)
    got_nx_next = send(nx_first, nx_next, "xln", False)
    got_bx_prev = send(bx_last, bx_prev, "xln", True)
    got_n_prev = send(n.at[top], n.at[0], "inl", True)
    got_n_next = send(n.at[1], n.at[end], "inl", False)
    got_b_prev = send(b.at[top], b.at[0], "inl", True)

    tail.wait()
    tail_n.wait()
    here, limit = n[top], b[top]
    dx = clip(SIGMA * (ahead(here, 0) - here), limit)
    dz = clip(SIGMA * (ahead(here, 1) - here), limit)
    dual[1, ni - 1] = dx
    dual[2, ni - 1] = dz
    div = (dx - behind(dx, 0)) - clip(SIGMA * (here - n[top - 1]), b[top - 1])
    div = div + (dz - behind(dz, 1))
    v[top] = here + (2.0 * GAIN) * div
    d1 = d1 + fold(dx * dx + dz * dz)
    d1 = lax.fori_loop(early, groups, pass_group, d1)
    for i in range(groups * GROUP, ni - 1):
        d1 = pass_one(i, d1)

    def no_prev(dst):
        def fill():
            dst[...] = jnp.zeros_like(dst)

        return fill

    def no_next(dst, low, high):
        def fill():
            dst[0:1] = low
            dst[1:2] = high

        return fill

    def grow(dst, rows, amount):
        dst[rows] = dst[rows] + (2.0 * GAIN) * amount

    got_zc_prev(no_prev(zc_prev))
    got_zc_next(no_next(zc_next, nx_first[last], nx_last[last]))
    grow(vx_first, first, -clip(SIGMA * (nx_first[first] - zc_prev[0:1]), zc_prev[2:3]))
    grow(vx_last, first, -clip(SIGMA * (nx_last[first] - zc_prev[1:2]), zc_prev[3:4]))
    grow(vx_first, last, clip(SIGMA * (zc_next[0:1] - nx_first[last]), bx_first[last]))
    grow(vx_last, last, clip(SIGMA * (zc_next[1:2] - nx_last[last]), bx_last[last]))
    got_vx_prev = send(vx_last, vx_prev, "xln", True)
    got_vx_next = send(vx_first, vx_next, "xln", False)
    got_xc_prev(no_prev(xc_prev))
    got_xc_next(no_next(xc_next, nx_last[first], nx_last[last]))
    for k, (rows, layer) in enumerate(((first, 1), (last, top))):
        outer = clip(SIGMA * (xc_next[k : k + 1] - nx_last[rows]), bx_last[rows])
        grow(v.at[layer], slice(nx - 1, nx), outer)
        outer = clip(SIGMA * (nx_first[rows] - xc_prev[k : k + 1]), xc_prev[2 + k : 3 + k])
        grow(v.at[layer], slice(0, 1), -outer)
    v_up = len(sent)
    got_v_prev = send(v.at[top], v.at[0], "inl", True)
    v_down = len(sent)
    got_v_next = send(v.at[1], v.at[end], "inl", False)

    if one_stage(ni_dev, nx_dev):
        for di in (2, -2):
            beyond = my_i - di // 2
            knows = jnp.logical_and(beyond >= 0, beyond < ni_dev)

            @pl.when(jnp.logical_and(knows, jnp.logical_and(my_i + di >= 0, my_i + di < ni_dev)))
            def _():
                pl.semaphore_signal(
                    far_sem, inc=1, device_id={"inl": my_i + di}, device_id_type=pl.DeviceIdType.MESH
                )

    row = lax.broadcasted_iota(jnp.int32, (8, nz), 0)

    def inner_rows(value, lo, hi):
        parts = split(value, 0, 8)
        if lo == 0:
            parts[0] = jnp.where(row == 0, 0.0, parts[0])
        if hi == nx:
            parts[-1] = jnp.where(row == 7, 0.0, parts[-1])
        return jnp.concatenate(parts, axis=0)

    def below(value, tile):
        turned = [pltpu.roll(part, 7, 0) for part in split(value, 0, 8)]
        over = [value[-8:] if tile is None else pltpu.roll(tile, 7, 0)]
        return jnp.concatenate([jnp.where(row == 7, x, t) for x, t in zip(turned[1:] + over, turned)], axis=0)

    def above(value, tile):
        turned = [pltpu.roll(part, 1, 0) for part in split(value, 0, 8)]
        under = [jnp.zeros_like(value[:8]) if tile is None else pltpu.roll(tile, 1, 0)]
        return jnp.concatenate([jnp.where(row == 0, x, t) for x, t in zip(under + turned[:-1], turned)], axis=0)

    def pass_two(i, so_far, lo=0, hi=nx, fresh=True):
        p1, p2, d2 = so_far
        here, limit, base = v[i + 1, lo:hi], b[i + 1, lo:hi], n[i + 1, lo:hi]
        oi, ox, oz = dual[0, i, lo:hi], dual[1, i, lo:hi], dual[2, i, lo:hi]
        di = clip(oi + SIGMA * (v[i + 2, lo:hi] - here), limit)
        dx = clip(ox + SIGMA * (below(here, v[i + 1, hi : hi + 8] if hi < nx else None) - here), limit)
        dz = clip(oz + SIGMA * (ahead(here, 1) - here), limit)
        if lo == 0:
            before = None
        elif fresh:
            before = v[i + 1, lo - 8 : lo]
            before = clip(dual[1, i, lo - 8 : lo] + SIGMA * (below(before, here[:8]) - before), b[i + 1, lo - 8 : lo])
        else:
            before = dual[1, i, lo - 8 : lo]
        dual[0, i, lo:hi] = di
        dual[1, i, lo:hi] = dx
        dual[2, i, lo:hi] = dz
        div = di - step[lo:hi]
        div = div + (dx - above(dx, before))
        div = div + (dz - behind(dz, 1))
        step[lo:hi] = di
        half = 0.5 * (here - base)
        change = GAIN * (div - half)
        out[i, lo:hi] = base + half + change
        inner = inner_rows(change, lo, hi)
        return (
            p1 + fold(half * half),
            p2 + fold(inner * inner),
            d2 + squares(di - oi, dx - ox, dz - oz),
        )

    def begin(lo, hi):
        step[lo:hi] = clip(
            dual[0, 1, lo:hi] + SIGMA * (v[3, lo:hi] - v[2, lo:hi]), b[2, lo:hi]
        )

    def middle(i, so_far):
        return pass_two(i, so_far, 8, nx - 8)

    def rim(i, so_far):
        return pass_two(i, pass_two(i, so_far, 0, 8), nx - 8, nx, False)

    begin(8, nx - 8)
    sums = stepped(2, ni - 2, middle, (zero,) * 3, MIDDLE)

    got_nx_prev(setter(nx_prev, nx_first))
    got_bx_prev(setter(bx_prev, bx_last))
    got_nx_next(setter(nx_next, nx_last))
    dx_last = clip(SIGMA * (nx_next[...] - nx_last[...]), bx_last[...])
    dxp = clip(SIGMA * (nx_first[...] - nx_prev[...]), bx_prev[...])
    dual[1, :, nx - 1, :] = dx_last
    dx_prev[...] = dxp
    dx_edge[...] = dx_last
    wx_last[...] = vx_last[...] + (2.0 * GAIN) * dx_last
    wx_first[...] = vx_first[...] - (2.0 * GAIN) * dxp
    v[2:top, nx - 1, :] = wx_last[1 : ni - 1]
    v[2:top, 0, :] = wx_first[1 : ni - 1]
    d1 = d1 + fold(dx_last * dx_last)

    begin(0, 8)
    begin(nx - 8, nx)
    sums = stepped(2, ni - 2, rim, sums, RIM)

    got_n_prev(setter(n.at[0], n.at[1]))
    got_b_prev(setter(b.at[0], b.at[1]))
    got_n_next(setter(n.at[end], n.at[top]))
    left(v_up)
    left(v_down)
    got_v_next(setter(v.at[end], v.at[top]))
    got_v_prev(setter(v.at[0], v.at[1]))
    di_last = clip(SIGMA * (n[end] - n[top]), b[top])
    dip = clip(SIGMA * (n[1] - n[0]), b[0])
    dual[0, ni - 1] = di_last
    d1 = d1 + fold(di_last * di_last)
    v[top] = v[top] + (2.0 * GAIN) * di_last
    v[1] = v[1] - (2.0 * GAIN) * dip
    v[end] = v[end] - (2.0 * GAIN) * di_last
    v[0] = v[0] + (2.0 * GAIN) * dip
    sums = pass_two(ni - 2, sums)
    sums = pass_two(ni - 1, sums)
    step[...] = clip(dip + SIGMA * (v[1] - v[0]), b[0])
    sums = pass_two(0, sums)
    p1, p2, d2 = pass_two(1, sums)

    got_vx_prev(setter(vx_prev, wx_first))
    got_vx_next(setter(vx_next, wx_last))
    was = dx_edge[...]
    dx_last = clip(
        was + SIGMA * (vx_next[...] - (2.0 * GAIN) * was - wx_last[...]), bx_last[...]
    )
    dual[1, :, nx - 1, :] = dx_last
    moved = dx_last - was
    d2 = d2 + fold(moved * moved)
    u_last = out[:, nx - 1, :] + GAIN * moved
    out[:, nx - 1, :] = u_last
    dxp = clip(
        dx_prev[...] + SIGMA * (wx_first[...] - (vx_prev[...] + (2.0 * GAIN) * dx_prev[...])), bx_prev[...]
    )
    u_first = out[:, 0, :] - GAIN * dxp
    out[:, 0, :] = u_first
    change = u_last - (nx_last[...] + 0.5 * (wx_last[...] - nx_last[...]))
    p2 = p2 + fold(change * change)
    change = u_first - (nx_first[...] + 0.5 * (wx_first[...] - nx_first[...]))
    p2 = p2 + fold(change * change)

    total = gather_lanes([jnp.sum(part, axis=0, keepdims=True) for part in (p1, d1, p2, d2)])
    if one_stage(ni_dev, nx_dev):
        far = 0
        for di in (3, -3):
            far = far + jnp.logical_and(my_i + di >= 0, my_i + di < ni_dev).astype(jnp.int32)
        if ni_dev > 3:
            @pl.when(far > 0)
            def _():
                pl.semaphore_wait(far_sem, 1)
    copies = []
    for stage, peers in enumerate(stages):
        mine[stage] = total
        first = len(copies)
        for k, (di, dx) in enumerate(peers, first):
            copy = pltpu.make_async_remote_copy(
                src_ref=mine.at[stage], dst_ref=others.at[k],
                send_sem=give_sem.at[k], recv_sem=take_sem.at[k],
                device_id=at(di, dx), device_id_type=pl.DeviceIdType.MESH,
            )
            copy.start()
            copies.append(copy)
        for k in range(first, len(copies)):
            copies[k].wait_recv()
            total = total + others[k]
    norms[...] = jnp.sqrt(jnp.concatenate([total, pltpu.roll(total, 126, 1)], axis=0)[:, 0:2])

    for copy in copies:
        copy.wait_send()
    for slot in range(len(sent)):
        if slot not in (v_up, v_down):
            left(slot)


def put_out(out_held, dual_held, norms_held, out, dual, norms, sems):
    half = out.shape[0] // 2
    pairs = [(norms_held, norms)]
    for at in (0, half):
        part = pl.ds(at, half)
        pairs.append((out_held.at[part], out.at[part]))
        for axis in range(3):
            pairs.append((dual_held.at[axis, part], dual.at[axis, part]))
    copies = [pltpu.make_async_copy(src, dst, sems.at[k]) for k, (src, dst) in enumerate(pairs)]
    for copy in copies:
        copy.start()
    for copy in copies:
        copy.wait()


def per_device(noisy, bound):
    ni, nx, nz = noisy.shape
    ni_dev, nx_dev = lax.axis_size("inl"), lax.axis_size("xln")
    f32 = jnp.float32
    face = pltpu.VMEM((ni, nz), f32)
    slab = pltpu.VMEM((nx, nz), f32)
    dma = pltpu.SemaphoreType.DMA
    volume = 4 * ni * nx * nz
    stages = reduction(ni_dev, nx_dev)
    peers = sum(len(stage) for stage in stages)
    noisy = pltpu.with_memory_space_constraint(noisy, pltpu.HBM)
    bound = pltpu.with_memory_space_constraint(bound, pltpu.HBM)
    held = pl.pallas_call(
        functools.partial(kernel, ni_dev, nx_dev),
        out_shape=(
            pltpu.VMEM((ni, nx, nz), f32),
            pltpu.VMEM((3, ni, nx, nz), f32),
            pltpu.VMEM((2, 2), f32),
        ),
        in_specs=[pl.BlockSpec(memory_space=pltpu.HBM)] * 2,
        out_specs=(
            pl.BlockSpec(memory_space=pltpu.VMEM),
            pl.BlockSpec(memory_space=pltpu.VMEM),
            pl.BlockSpec(memory_space=pltpu.VMEM),
        ),
        scratch_shapes=[
            pltpu.VMEM((ni + 2, nx, nz), f32),
            pltpu.VMEM((ni + 1, nx, nz), f32),
            pltpu.VMEM((ni + 2, nx, nz), f32),
            slab,
            *([face] * 18),
            *([pltpu.VMEM((4, nz), f32), pltpu.VMEM((2, nz), f32)] * 4),
            pltpu.VMEM((len(stages), 1, 128), f32),
            pltpu.VMEM((peers, 1, 128), f32),
            dma((10,)), dma((2, (ni - 1) // GROUP + 1)), dma((14,)), dma((14,)), dma((peers,)), dma((peers,)),
            pltpu.SemaphoreType.REGULAR,
        ],
        compiler_params=pltpu.CompilerParams(
            collective_id=0, has_side_effects=True, vmem_limit_bytes=24 * 1024 * 1024
        ),
        cost_estimate=pl.CostEstimate(
            flops=80 * ni * nx * nz, bytes_accessed=6 * volume, transcendentals=0
        ),
        name="denoise",
    )(noisy, bound)
    in_vmem = pl.BlockSpec(memory_space=pltpu.VMEM)
    in_hbm = pl.BlockSpec(memory_space=pltpu.HBM)
    return pl.pallas_call(
        put_out,
        out_shape=(
            jax.ShapeDtypeStruct((ni, nx, nz), f32),
            jax.ShapeDtypeStruct((3, ni, nx, nz), f32),
            jax.ShapeDtypeStruct((2, 2), f32),
        ),
        in_specs=[in_vmem] * 3,
        out_specs=(in_hbm,) * 3,
        scratch_shapes=[dma((9,))],
        compiler_params=pltpu.CompilerParams(vmem_limit_bytes=1024 * 1024),
        cost_estimate=pl.CostEstimate(flops=0, bytes_accessed=4 * volume, transcendentals=0),
        name="put_out",
    )(*held)


def solution(mesh):
    in_specs = (P("inl", "xln", None), P("inl", "xln", None))
    out_specs = (P("inl", "xln", None), P(None, "inl", "xln", None), P())
    return jax.shard_map(
        per_device, mesh=mesh, in_specs=in_specs, out_specs=out_specs, check_vma=False
    )
```

```python
import functools

import jax
import jax.numpy as jnp
from jax import lax
from jax.experimental import pallas as pl
from jax.experimental.pallas import tpu as pltpu
from jax.sharding import PartitionSpec as P

SIGMA = 0.28
TAU = 0.28
GAIN = TAU / (1.0 + TAU)
GROUP = 4
AHEAD = 1
EARLY = 1
MIDDLE = 7
RIM = 7


def clip(value, limit):
    return jnp.minimum(jnp.maximum(value, -limit), limit)


def fold(square):
    rows, lanes = square.shape
    total = square[0:8]
    for at in range(8, rows, 8):
        total = total + square[at : at + 8]
    part = total[:, 0:128]
    for at in range(128, lanes, 128):
        part = part + total[:, at : at + 128]
    return part


def gather_lanes(parts):
    lane = lax.broadcasted_iota(jnp.int32, (2, 128), 1)
    row = lax.broadcasted_iota(jnp.int32, (2, 128), 0)
    result = jnp.zeros((2, 128), jnp.float32)
    for k, part in enumerate(parts):
        total = jnp.sum(jnp.sum(part, axis=0, keepdims=True), axis=1, keepdims=True)
        result = jnp.where(jnp.logical_and(row == k // 2, lane == k % 2), total, result)
    return result


def one_stage(ni_dev, nx_dev):
    return ni_dev <= 4 and ni_dev * nx_dev <= 32


def reduction(ni_dev, nx_dev):
    everyone = [(di, dx) for di in range(ni_dev) for dx in range(nx_dev) if di or dx]
    if one_stage(ni_dev, nx_dev):
        return [everyone]
    return [[peer for peer in everyone if peer[0] == 0], [peer for peer in everyone if peer[1] == 0]]


def stepped(start, stop, body, carry, unroll=4):
    def group(k, carry):
        for at in range(unroll):
            carry = body(start + k * unroll + at, carry)
        return carry

    whole = (stop - start) // unroll
    carry = lax.fori_loop(0, whole, group, carry)
    for i in range(start + whole * unroll, stop):
        carry = body(i, carry)
    return carry


def split(value, dim, size):
    return [lax.slice_in_dim(value, at, at + size, axis=dim) for at in range(0, value.shape[dim], size)]


def ahead(value, dim):
    size = (8, 128)[dim]
    parts = split(value, dim, size)
    turned = [pltpu.roll(part, size - 1, dim) for part in parts]
    edge = lax.broadcasted_iota(jnp.int32, parts[0].shape, dim) == size - 1
    after = turned[1:] + [parts[-1]]
    return jnp.concatenate([jnp.where(edge, a, t) for a, t in zip(after, turned)], axis=dim)


def behind(value, dim):
    size = (8, 128)[dim]
    turned = [pltpu.roll(part, 1, dim) for part in split(value, dim, size)]
    edge = lax.broadcasted_iota(jnp.int32, turned[0].shape, dim) == 0
    before = [jnp.zeros_like(turned[0])] + turned[:-1]
    return jnp.concatenate([jnp.where(edge, a, t) for a, t in zip(before, turned)], axis=dim)


def kernel(
    ni_dev, nx_dev,
    noisy, bound, out, dual, norms,
    n, b, v, step,
    nx_first, nx_last, bx_last, bx_first, nx_second, nx_semi, bx_semi,
    nx_next, nx_prev, bx_prev,
    vx_first, vx_last, vx_next, vx_prev, wx_first, wx_last, dx_prev, dx_edge, di_prev,
    zc_up, zc_down, zc_prev, zc_next, xc_up, xc_down, xc_prev, xc_next,
    mine, others,
    load_sem, chunk_sem, send_sem, recv_sem, give_sem, take_sem, far_sem,
):
    ni, nx, nz = noisy.shape
    top, end = ni, ni + 1
    my_i, my_x = lax.axis_index("inl"), lax.axis_index("xln")
    f32 = jnp.float32

    barrier = pltpu.get_barrier_semaphore()
    stages = reduction(ni_dev, nx_dev)

    def at(di, dx):
        return {"inl": lax.rem(my_i + di, ni_dev), "xln": lax.rem(my_x + dx, nx_dev)}

    hello = [(di, 0) for di in range(1 - ni_dev, ni_dev) if di and (abs(di) == 1 or not one_stage(ni_dev, nx_dev))]
    hello = sorted(hello, key=lambda peer: abs(peer[0])) + [(0, dx) for dx in range(1, nx_dev)]
    greeted = 0
    for di, dx in hello:
        exists = jnp.logical_and(my_i + di >= 0, my_i + di < ni_dev)
        greeted = greeted + exists.astype(jnp.int32)

        @pl.when(exists)
        def _():
            pl.semaphore_signal(
                barrier, inc=1,
                device_id={"inl": my_i + di, "xln": lax.rem(my_x + dx, nx_dev)},
                device_id_type=pl.DeviceIdType.MESH,
            )

    loads = []

    def load(src, dst):
        copy = pltpu.make_async_copy(src, dst, load_sem.at[len(loads)])
        copy.start()
        loads.append(copy)

    def chunk(k, size):
        return (
            pltpu.make_async_copy(
                noisy.at[pl.ds(GROUP * k + 1, size)], n.at[pl.ds(GROUP * k + 2, size)], chunk_sem.at[0, k]
            ),
            pltpu.make_async_copy(
                bound.at[pl.ds(GROUP * k, size)], b.at[pl.ds(GROUP * k + 1, size)], chunk_sem.at[1, k]
            ),
        )

    groups = (ni - 1) // GROUP
    rest = ni - 1 - groups * GROUP
    pieces = [(k, GROUP) for k in range(groups)]
    tail = pltpu.make_async_copy(
        bound.at[pl.ds(ni - 1 - rest, rest)], b.at[pl.ds(ni - rest, rest)], chunk_sem.at[1, groups]
    )
    tail_n = pltpu.make_async_copy(
        noisy.at[pl.ds(ni - rest, rest - 1)], n.at[pl.ds(ni - rest + 1, rest - 1)], chunk_sem.at[0, groups]
    )
    load(noisy.at[pl.ds(0, 1)], n.at[pl.ds(1, 1)])
    for k, size in pieces[:AHEAD]:
        for copy in chunk(k, size):
            copy.start()
    load(noisy.at[:, 0, :], nx_first)
    load(noisy.at[:, nx - 1, :], nx_last)
    load(bound.at[:, nx - 1, :], bx_last)
    load(bound.at[:, 0, :], bx_first)
    load(noisy.at[pl.ds(ni - 1, 1)], n.at[pl.ds(top, 1)])
    load(bound.at[pl.ds(ni - 1, 1)], b.at[pl.ds(top, 1)])
    load(noisy.at[:, 1, :], nx_second)
    load(noisy.at[:, nx - 2, :], nx_semi)
    load(bound.at[:, nx - 2, :], bx_semi)
    for k, size in pieces[AHEAD:]:
        for copy in chunk(k, size):
            copy.start()
    tail.start()
    tail_n.start()

    sent = []

    def send(src, dst, axis, forward):
        slot = len(sent)
        me, count = (my_i, ni_dev) if axis == "inl" else (my_x, nx_dev)
        target = lax.rem(me + (1 if forward else count - 1), count)
        copy = pltpu.make_async_remote_copy(
            src_ref=src, dst_ref=dst, send_sem=send_sem.at[slot], recv_sem=recv_sem.at[slot],
            device_id={axis: target}, device_id_type=pl.DeviceIdType.MESH,
        )
        not_last, not_first = me < count - 1, me > 0
        can_send, can_recv = (not_last, not_first) if forward else (not_first, not_last)

        @pl.when(can_send)
        def _():
            copy.start()

        sent.append((copy, can_send))

        def arrive(fill):
            @pl.when(can_recv)
            def _():
                copy.wait_recv()

            @pl.when(jnp.logical_not(can_recv))
            def _():
                fill()

        return arrive

    def left(slot):
        copy, can_send = sent[slot]

        @pl.when(can_send)
        def _():
            copy.wait_send()

    def setter(dst, src):
        def fill():
            dst[...] = src[...]

        return fill

    first, last = slice(0, 1), slice(ni - 1, ni)

    step[...] = jnp.zeros_like(step)

    def squares(oi, ox, oz):
        return fold(oi * oi + ox * ox + oz * oz)

    def pass_one(i, d1):
        here, limit = n[i + 1], b[i + 1]
        di = clip(SIGMA * (n[i + 2] - here), limit)
        dx = clip(SIGMA * (ahead(here, 0) - here), limit)
        dz = clip(SIGMA * (ahead(here, 1) - here), limit)
        dual[0, i] = di
        dual[1, i] = dx
        dual[2, i] = dz
        div = di - step[...]
        div = div + (dx - behind(dx, 0))
        div = div + (dz - behind(dz, 1))
        step[...] = di
        v[i + 1] = here + (2.0 * GAIN) * div
        return d1 + squares(di, dx, dz)

    zero = jnp.zeros((8, 128), jnp.float32)

    def pass_group(k, d1):
        for copy in chunk(k, GROUP):
            copy.wait()
        for at in range(GROUP):
            d1 = pass_one(GROUP * k + at, d1)
        return d1

    early = min(EARLY, groups)
    loads[0].wait()
    d1 = lax.fori_loop(0, early, pass_group, zero)
    for k in range(1, 10):
        loads[k].wait()
    zc_up[0:1], zc_up[1:2], zc_up[2:3], zc_up[3:4] = nx_first[last], nx_last[last], bx_first[last], bx_last[last]
    zc_down[0:1], zc_down[1:2] = nx_first[first], nx_last[first]
    xc_up[0:1], xc_up[1:2], xc_up[2:3], xc_up[3:4] = nx_last[first], nx_last[last], bx_last[first], bx_last[last]
    xc_down[0:1], xc_down[1:2] = nx_first[first], nx_first[last]
    pl.semaphore_wait(barrier, greeted)
    got_zc_prev = send(zc_up, zc_prev, "inl", True)
    got_zc_next = send(zc_down, zc_next, "inl", False)
    got_xc_prev = send(xc_up, xc_prev, "xln", True)
    got_xc_next = send(xc_down, xc_next, "xln", False)
    got_n_prev = send(n.at[top], n.at[0], "inl", True)
    got_n_next = send(n.at[1], n.at[end], "inl", False)
    got_b_prev = send(b.at[top], b.at[0], "inl", True)
    got_nx_prev = send(nx_last, nx_prev, "xln", True)
    got_nx_next = send(nx_first, nx_next, "xln", False)
    got_bx_prev = send(bx_last, bx_prev, "xln", True)

    def edge(here, limit, side):
        di = clip(SIGMA * (ahead(here, 0) - here), limit)
        dz = clip(SIGMA * (ahead(here, 1) - here), limit)
        return here + (2.0 * GAIN) * ((di - behind(di, 0)) + side + (dz - behind(dz, 1)))

    inward = clip(SIGMA * (nx_second[...] - nx_first[...]), bx_first[...])
    vx_first[...] = edge(nx_first[...], bx_first[...], inward)
    inward = clip(SIGMA * (nx_last[...] - nx_semi[...]), bx_semi[...])
    vx_last[...] = edge(nx_last[...], bx_last[...], -inward)

    d1 = lax.fori_loop(early, groups, pass_group, d1)
    tail.wait()
    tail_n.wait()
    here, limit = n[top], b[top]
    dx = clip(SIGMA * (ahead(here, 0) - here), limit)
    dz = clip(SIGMA * (ahead(here, 1) - here), limit)
    dual[1, ni - 1] = dx
    dual[2, ni - 1] = dz
    div = (dx - behind(dx, 0)) - clip(SIGMA * (here - n[top - 1]), b[top - 1])
    div = div + (dz - behind(dz, 1))
    v[top] = here + (2.0 * GAIN) * div
    d1 = d1 + fold(dx * dx + dz * dz)
    for i in range(groups * GROUP, ni - 1):
        d1 = pass_one(i, d1)

    def no_prev(dst):
        def fill():
            dst[...] = jnp.zeros_like(dst)

        return fill

    def no_next(dst, low, high):
        def fill():
            dst[0:1] = low
            dst[1:2] = high

        return fill

    def grow(dst, rows, amount):
        dst[rows] = dst[rows] + (2.0 * GAIN) * amount

    got_zc_prev(no_prev(zc_prev))
    got_zc_next(no_next(zc_next, nx_first[last], nx_last[last]))
    grow(vx_first, first, -clip(SIGMA * (nx_first[first] - zc_prev[0:1]), zc_prev[2:3]))
    grow(vx_last, first, -clip(SIGMA * (nx_last[first] - zc_prev[1:2]), zc_prev[3:4]))
    grow(vx_first, last, clip(SIGMA * (zc_next[0:1] - nx_first[last]), bx_first[last]))
    grow(vx_last, last, clip(SIGMA * (zc_next[1:2] - nx_last[last]), bx_last[last]))
    got_vx_prev = send(vx_last, vx_prev, "xln", True)
    got_vx_next = send(vx_first, vx_next, "xln", False)
    got_xc_prev(no_prev(xc_prev))
    got_xc_next(no_next(xc_next, nx_last[first], nx_last[last]))
    for k, (rows, layer) in enumerate(((first, 1), (last, top))):
        outer = clip(SIGMA * (xc_next[k : k + 1] - nx_last[rows]), bx_last[rows])
        grow(v.at[layer], slice(nx - 1, nx), outer)
        outer = clip(SIGMA * (nx_first[rows] - xc_prev[k : k + 1]), xc_prev[2 + k : 3 + k])
        grow(v.at[layer], slice(0, 1), -outer)
    v_up = len(sent)
    got_v_prev = send(v.at[top], v.at[0], "inl", True)
    v_down = len(sent)
    got_v_next = send(v.at[1], v.at[end], "inl", False)

    if one_stage(ni_dev, nx_dev):
        for di in (2, -2):
            beyond = my_i - di // 2
            knows = jnp.logical_and(beyond >= 0, beyond < ni_dev)

            @pl.when(jnp.logical_and(knows, jnp.logical_and(my_i + di >= 0, my_i + di < ni_dev)))
            def _():
                pl.semaphore_signal(
                    far_sem, inc=1, device_id={"inl": my_i + di}, device_id_type=pl.DeviceIdType.MESH
                )

    row = lax.broadcasted_iota(jnp.int32, (8, nz), 0)

    def inner_rows(value, lo, hi):
        parts = split(value, 0, 8)
        if lo == 0:
            parts[0] = jnp.where(row == 0, 0.0, parts[0])
        if hi == nx:
            parts[-1] = jnp.where(row == 7, 0.0, parts[-1])
        return jnp.concatenate(parts, axis=0)

    def below(value, tile):
        turned = [pltpu.roll(part, 7, 0) for part in split(value, 0, 8)]
        over = [value[-8:] if tile is None else pltpu.roll(tile, 7, 0)]
        return jnp.concatenate([jnp.where(row == 7, x, t) for x, t in zip(turned[1:] + over, turned)], axis=0)

    def above(value, tile):
        turned = [pltpu.roll(part, 1, 0) for part in split(value, 0, 8)]
        under = [jnp.zeros_like(value[:8]) if tile is None else pltpu.roll(tile, 1, 0)]
        return jnp.concatenate([jnp.where(row == 0, x, t) for x, t in zip(under + turned[:-1], turned)], axis=0)

    def pass_two(i, so_far, lo=0, hi=nx, fresh=True):
        p1, p2, d2 = so_far
        here, limit, base = v[i + 1, lo:hi], b[i + 1, lo:hi], n[i + 1, lo:hi]
        oi, ox, oz = dual[0, i, lo:hi], dual[1, i, lo:hi], dual[2, i, lo:hi]
        di = clip(oi + SIGMA * (v[i + 2, lo:hi] - here), limit)
        dx = clip(ox + SIGMA * (below(here, v[i + 1, hi : hi + 8] if hi < nx else None) - here), limit)
        dz = clip(oz + SIGMA * (ahead(here, 1) - here), limit)
        if lo == 0:
            before = None
        elif fresh:
            before = v[i + 1, lo - 8 : lo]
            before = clip(dual[1, i, lo - 8 : lo] + SIGMA * (below(before, here[:8]) - before), b[i + 1, lo - 8 : lo])
        else:
            before = dual[1, i, lo - 8 : lo]
        dual[0, i, lo:hi] = di
        dual[1, i, lo:hi] = dx
        dual[2, i, lo:hi] = dz
        div = di - step[lo:hi]
        div = div + (dx - above(dx, before))
        div = div + (dz - behind(dz, 1))
        step[lo:hi] = di
        half = 0.5 * (here - base)
        change = GAIN * (div - half)
        out[i, lo:hi] = base + half + change
        inner = inner_rows(change, lo, hi)
        return (
            p1 + fold(half * half),
            p2 + fold(inner * inner),
            d2 + squares(di - oi, dx - ox, dz - oz),
        )

    def begin(lo, hi):
        step[lo:hi] = clip(
            dual[0, 1, lo:hi] + SIGMA * (v[3, lo:hi] - v[2, lo:hi]), b[2, lo:hi]
        )

    def middle(i, so_far):
        return pass_two(i, so_far, 8, nx - 8)

    def rim(i, so_far):
        return pass_two(i, pass_two(i, so_far, 0, 8), nx - 8, nx, False)

    begin(8, nx - 8)
    sums = stepped(2, ni - 2, middle, (zero,) * 3, MIDDLE)

    got_nx_prev(setter(nx_prev, nx_first))
    got_bx_prev(setter(bx_prev, bx_last))
    got_nx_next(setter(nx_next, nx_last))
    dx_last = clip(SIGMA * (nx_next[...] - nx_last[...]), bx_last[...])
    dxp = clip(SIGMA * (nx_first[...] - nx_prev[...]), bx_prev[...])
    dual[1, :, nx - 1, :] = dx_last
    dx_prev[...] = dxp
    dx_edge[...] = dx_last
    wx_last[...] = vx_last[...] + (2.0 * GAIN) * dx_last
    wx_first[...] = vx_first[...] - (2.0 * GAIN) * dxp
    v[2:top, nx - 1, :] = wx_last[1 : ni - 1]
    v[2:top, 0, :] = wx_first[1 : ni - 1]
    d1 = d1 + fold(dx_last * dx_last)

    begin(0, 8)
    begin(nx - 8, nx)
    sums = stepped(2, ni - 2, rim, sums, RIM)

    got_n_prev(setter(n.at[0], n.at[1]))
    got_b_prev(setter(b.at[0], b.at[1]))
    got_n_next(setter(n.at[end], n.at[top]))
    left(v_up)
    left(v_down)
    di_last = clip(SIGMA * (n[end] - n[top]), b[top])
    dip = clip(SIGMA * (n[1] - n[0]), b[0])
    dual[0, ni - 1] = di_last
    di_prev[...] = dip
    d1 = d1 + fold(di_last * di_last)
    v[top] = v[top] + (2.0 * GAIN) * di_last
    v[1] = v[1] - (2.0 * GAIN) * dip
    sums = pass_two(ni - 2, sums)
    step[...] = clip(dual[0, 0] + SIGMA * (v[2] - v[1]), b[1])
    sums = pass_two(1, sums)

    got_vx_prev(setter(vx_prev, wx_first))
    got_vx_next(setter(vx_next, wx_last))
    got_v_next(setter(v.at[end], v.at[top]))
    got_v_prev(setter(v.at[0], v.at[1]))
    v[end] = v[end] - (2.0 * GAIN) * dual[0, ni - 1]
    v[0] = v[0] + (2.0 * GAIN) * di_prev[...]
    step[...] = dual[0, ni - 2]
    sums = pass_two(ni - 1, sums)
    step[...] = clip(di_prev[...] + SIGMA * (v[1] - v[0]), b[0])
    p1, p2, d2 = pass_two(0, sums)

    was = dx_edge[...]
    dx_last = clip(
        was + SIGMA * (vx_next[...] - (2.0 * GAIN) * was - wx_last[...]), bx_last[...]
    )
    dual[1, :, nx - 1, :] = dx_last
    moved = dx_last - was
    d2 = d2 + fold(moved * moved)
    u_last = out[:, nx - 1, :] + GAIN * moved
    out[:, nx - 1, :] = u_last
    dxp = clip(
        dx_prev[...] + SIGMA * (wx_first[...] - (vx_prev[...] + (2.0 * GAIN) * dx_prev[...])), bx_prev[...]
    )
    u_first = out[:, 0, :] - GAIN * dxp
    out[:, 0, :] = u_first
    change = u_last - (nx_last[...] + 0.5 * (wx_last[...] - nx_last[...]))
    p2 = p2 + fold(change * change)
    change = u_first - (nx_first[...] + 0.5 * (wx_first[...] - nx_first[...]))
    p2 = p2 + fold(change * change)

    total = gather_lanes((p1, d1, p2, d2))
    if one_stage(ni_dev, nx_dev):
        far = 0
        for di in (3, -3):
            far = far + jnp.logical_and(my_i + di >= 0, my_i + di < ni_dev).astype(jnp.int32)
        if ni_dev > 3:
            @pl.when(far > 0)
            def _():
                pl.semaphore_wait(far_sem, 1)
    first = 0
    waits = []
    for stage, peers in enumerate(stages):
        mine[stage] = total
        for k, (di, dx) in enumerate(peers, first):
            pltpu.make_async_remote_copy(
                src_ref=mine.at[stage], dst_ref=others.at[k],
                send_sem=give_sem.at[stage], recv_sem=take_sem.at[stage],
                device_id=at(di, dx), device_id_type=pl.DeviceIdType.MESH,
            ).start()
        landed = others.at[pl.ds(first, len(peers))]
        pltpu.make_async_copy(landed, landed, take_sem.at[stage]).wait()
        waits.append(pltpu.make_async_copy(landed, landed, give_sem.at[stage]))
        rows = [total] + [others[k] for k in range(first, first + len(peers))]
        while len(rows) > 1:
            rows = [sum(rows[k + 1 : k + 2], rows[k]) for k in range(0, len(rows), 2)]
        total = rows[0]
        first += len(peers)
    norms[...] = jnp.sqrt(total[:, 0:2])

    for copy in waits:
        copy.wait()
    for slot in range(len(sent)):
        if slot not in (v_up, v_down):
            left(slot)


def put_out(out_held, dual_held, norms_held, out, dual, norms, sems):
    half = out.shape[0] // 2
    pairs = [(norms_held, norms)]
    for at in (0, half):
        part = pl.ds(at, half)
        pairs.append((out_held.at[part], out.at[part]))
        for axis in range(3):
            pairs.append((dual_held.at[axis, part], dual.at[axis, part]))
    copies = [pltpu.make_async_copy(src, dst, sems.at[k]) for k, (src, dst) in enumerate(pairs)]
    for copy in copies:
        copy.start()
    for copy in copies:
        copy.wait()


def per_device(noisy, bound):
    ni, nx, nz = noisy.shape
    ni_dev, nx_dev = lax.axis_size("inl"), lax.axis_size("xln")
    f32 = jnp.float32
    face = pltpu.VMEM((ni, nz), f32)
    slab = pltpu.VMEM((nx, nz), f32)
    dma = pltpu.SemaphoreType.DMA
    volume = 4 * ni * nx * nz
    stages = reduction(ni_dev, nx_dev)
    peers = sum(len(stage) for stage in stages)
    noisy = pltpu.with_memory_space_constraint(noisy, pltpu.HBM)
    bound = pltpu.with_memory_space_constraint(bound, pltpu.HBM)
    held = pl.pallas_call(
        functools.partial(kernel, ni_dev, nx_dev),
        out_shape=(
            pltpu.VMEM((ni, nx, nz), f32),
            pltpu.VMEM((3, ni, nx, nz), f32),
            pltpu.VMEM((2, 2), f32),
        ),
        in_specs=[pl.BlockSpec(memory_space=pltpu.HBM)] * 2,
        out_specs=(
            pl.BlockSpec(memory_space=pltpu.VMEM),
            pl.BlockSpec(memory_space=pltpu.VMEM),
            pl.BlockSpec(memory_space=pltpu.VMEM),
        ),
        scratch_shapes=[
            pltpu.VMEM((ni + 2, nx, nz), f32),
            pltpu.VMEM((ni + 1, nx, nz), f32),
            pltpu.VMEM((ni + 2, nx, nz), f32),
            slab,
            *([face] * 18),
            slab,
            *([pltpu.VMEM((4, nz), f32), pltpu.VMEM((2, nz), f32)] * 4),
            pltpu.VMEM((len(stages), 2, 128), f32),
            pltpu.VMEM((peers, 2, 128), f32),
            dma((10,)), dma((2, (ni - 1) // GROUP + 1)), dma((14,)), dma((14,)), dma((len(stages),)), dma((len(stages),)),
            pltpu.SemaphoreType.REGULAR,
        ],
        compiler_params=pltpu.CompilerParams(
            collective_id=0, has_side_effects=True, vmem_limit_bytes=24 * 1024 * 1024
        ),
        cost_estimate=pl.CostEstimate(
            flops=80 * ni * nx * nz, bytes_accessed=6 * volume, transcendentals=0
        ),
        name="denoise",
    )(noisy, bound)
    in_vmem = pl.BlockSpec(memory_space=pltpu.VMEM)
    in_hbm = pl.BlockSpec(memory_space=pltpu.HBM)
    return pl.pallas_call(
        put_out,
        out_shape=(
            jax.ShapeDtypeStruct((ni, nx, nz), f32),
            jax.ShapeDtypeStruct((3, ni, nx, nz), f32),
            jax.ShapeDtypeStruct((2, 2), f32),
        ),
        in_specs=[in_vmem] * 3,
        out_specs=(in_hbm,) * 3,
        scratch_shapes=[dma((9,))],
        compiler_params=pltpu.CompilerParams(vmem_limit_bytes=1024 * 1024),
        cost_estimate=pl.CostEstimate(flops=0, bytes_accessed=4 * volume, transcendentals=0),
        name="put_out",
    )(*held)


def solution(mesh):
    in_specs = (P("inl", "xln", None), P("inl", "xln", None))
    out_specs = (P("inl", "xln", None), P(None, "inl", "xln", None), P())
    return jax.shard_map(
        per_device, mesh=mesh, in_specs=in_specs, out_specs=out_specs, check_vma=False
    )
```

```python
import functools

import jax
import jax.numpy as jnp
from jax import lax
from jax.experimental import pallas as pl
from jax.experimental.pallas import tpu as pltpu
from jax.sharding import PartitionSpec as P

SIGMA = 0.28
TAU = 0.28
GAIN = TAU / (1.0 + TAU)
GROUP = 4
AHEAD = 1
EARLY = 1
MIDDLE = 7
RIM = 7


def clip(value, limit):
    return jnp.minimum(jnp.maximum(value, -limit), limit)


def fold(square):
    rows, lanes = square.shape
    total = square[0:8]
    for at in range(8, rows, 8):
        total = total + square[at : at + 8]
    part = total[:, 0:128]
    for at in range(128, lanes, 128):
        part = part + total[:, at : at + 128]
    return part


def gather_lanes(parts):
    lane = lax.broadcasted_iota(jnp.int32, (2, 128), 1)
    row = lax.broadcasted_iota(jnp.int32, (2, 128), 0)
    result = jnp.zeros((2, 128), jnp.float32)
    for k, part in enumerate(parts):
        total = jnp.sum(jnp.sum(part, axis=0, keepdims=True), axis=1, keepdims=True)
        result = jnp.where(jnp.logical_and(row == k // 2, lane == k % 2), total, result)
    return result


def one_stage(ni_dev, nx_dev):
    return ni_dev <= 4 and ni_dev * nx_dev <= 32


def reduction(ni_dev, nx_dev):
    around = [[*range(1, count), 0] for count in (ni_dev, nx_dev)]
    everyone = [(di, dx) for di in around[0] for dx in around[1] if di or dx]
    if one_stage(ni_dev, nx_dev):
        return [everyone]
    return [[peer for peer in everyone if peer[0] == 0], [peer for peer in everyone if peer[1] == 0]]


def stepped(start, stop, body, carry, unroll=4):
    def group(k, carry):
        for at in range(unroll):
            carry = body(start + k * unroll + at, carry)
        return carry

    whole = (stop - start) // unroll
    carry = lax.fori_loop(0, whole, group, carry)
    for i in range(start + whole * unroll, stop):
        carry = body(i, carry)
    return carry


def split(value, dim, size):
    return [lax.slice_in_dim(value, at, at + size, axis=dim) for at in range(0, value.shape[dim], size)]


def ahead(value, dim):
    size = (8, 128)[dim]
    parts = split(value, dim, size)
    turned = [pltpu.roll(part, size - 1, dim) for part in parts]
    edge = lax.broadcasted_iota(jnp.int32, parts[0].shape, dim) == size - 1
    after = turned[1:] + [parts[-1]]
    return jnp.concatenate([jnp.where(edge, a, t) for a, t in zip(after, turned)], axis=dim)


def behind(value, dim):
    size = (8, 128)[dim]
    turned = [pltpu.roll(part, 1, dim) for part in split(value, dim, size)]
    edge = lax.broadcasted_iota(jnp.int32, turned[0].shape, dim) == 0
    before = [jnp.zeros_like(turned[0])] + turned[:-1]
    return jnp.concatenate([jnp.where(edge, a, t) for a, t in zip(before, turned)], axis=dim)


def kernel(
    ni_dev, nx_dev,
    noisy, bound, out, dual, norms,
    n, b, v, step,
    nx_first, nx_last, bx_last, bx_first, nx_second, nx_semi, bx_semi,
    nx_next, nx_prev, bx_prev,
    vx_first, vx_last, vx_next, vx_prev, wx_first, wx_last, dx_prev, dx_edge, di_prev,
    zc_up, zc_down, zc_prev, zc_next, xc_up, xc_down, xc_prev, xc_next,
    mine, others,
    load_sem, chunk_sem, send_sem, recv_sem, give_sem, take_sem, far_sem,
):
    ni, nx, nz = noisy.shape
    top, end = ni, ni + 1
    my_i, my_x = lax.axis_index("inl"), lax.axis_index("xln")
    f32 = jnp.float32

    barrier = pltpu.get_barrier_semaphore()
    stages = reduction(ni_dev, nx_dev)

    def at(di, dx):
        return {"inl": lax.rem(my_i + di, ni_dev), "xln": lax.rem(my_x + dx, nx_dev)}

    loads = []

    def load(src, dst):
        copy = pltpu.make_async_copy(src, dst, load_sem.at[len(loads)])
        copy.start()
        loads.append(copy)

    def chunk(k, size):
        return (
            pltpu.make_async_copy(
                noisy.at[pl.ds(GROUP * k + 1, size)], n.at[pl.ds(GROUP * k + 2, size)], chunk_sem.at[0, k]
            ),
            pltpu.make_async_copy(
                bound.at[pl.ds(GROUP * k, size)], b.at[pl.ds(GROUP * k + 1, size)], chunk_sem.at[1, k]
            ),
        )

    groups = (ni - 1) // GROUP
    rest = ni - 1 - groups * GROUP
    pieces = [(k, GROUP) for k in range(groups)]
    tail = pltpu.make_async_copy(
        bound.at[pl.ds(ni - 1 - rest, rest)], b.at[pl.ds(ni - rest, rest)], chunk_sem.at[1, groups]
    )
    tail_n = pltpu.make_async_copy(
        noisy.at[pl.ds(ni - rest, rest - 1)], n.at[pl.ds(ni - rest + 1, rest - 1)], chunk_sem.at[0, groups]
    )
    load(noisy.at[pl.ds(0, 1)], n.at[pl.ds(1, 1)])
    for k, size in pieces[:AHEAD]:
        for copy in chunk(k, size):
            copy.start()
    hello = [(di, 0) for di in range(1 - ni_dev, ni_dev) if di and (abs(di) == 1 or not one_stage(ni_dev, nx_dev))]
    hello = sorted(hello, key=lambda peer: abs(peer[0])) + [(0, dx) for dx in range(1, nx_dev)]
    greeted = 0
    for di, dx in hello:
        exists = jnp.logical_and(my_i + di >= 0, my_i + di < ni_dev)
        greeted = greeted + exists.astype(jnp.int32)

        @pl.when(exists)
        def _():
            pl.semaphore_signal(
                barrier, inc=1,
                device_id={"inl": my_i + di, "xln": lax.rem(my_x + dx, nx_dev)},
                device_id_type=pl.DeviceIdType.MESH,
            )

    load(noisy.at[:, 0, :], nx_first)
    load(noisy.at[:, nx - 1, :], nx_last)
    load(bound.at[:, nx - 1, :], bx_last)
    load(bound.at[:, 0, :], bx_first)
    load(noisy.at[pl.ds(ni - 1, 1)], n.at[pl.ds(top, 1)])
    load(bound.at[pl.ds(ni - 1, 1)], b.at[pl.ds(top, 1)])
    load(noisy.at[:, 1, :], nx_second)
    load(noisy.at[:, nx - 2, :], nx_semi)
    load(bound.at[:, nx - 2, :], bx_semi)
    for k, size in pieces[AHEAD:]:
        for copy in chunk(k, size):
            copy.start()
    tail.start()
    tail_n.start()

    sent = []

    def send(src, dst, axis, forward):
        slot = len(sent)
        me, count = (my_i, ni_dev) if axis == "inl" else (my_x, nx_dev)
        target = lax.rem(me + (1 if forward else count - 1), count)
        copy = pltpu.make_async_remote_copy(
            src_ref=src, dst_ref=dst, send_sem=send_sem.at[slot], recv_sem=recv_sem.at[slot],
            device_id={axis: target}, device_id_type=pl.DeviceIdType.MESH,
        )
        not_last, not_first = me < count - 1, me > 0
        can_send, can_recv = (not_last, not_first) if forward else (not_first, not_last)

        @pl.when(can_send)
        def _():
            copy.start()

        sent.append((copy, can_send))

        def arrive(fill):
            @pl.when(can_recv)
            def _():
                copy.wait_recv()

            @pl.when(jnp.logical_not(can_recv))
            def _():
                fill()

        return arrive

    def left(slot):
        copy, can_send = sent[slot]

        @pl.when(can_send)
        def _():
            copy.wait_send()

    def setter(dst, src):
        def fill():
            dst[...] = src[...]

        return fill

    first, last = slice(0, 1), slice(ni - 1, ni)

    step[...] = jnp.zeros_like(step)

    def squares(oi, ox, oz):
        return fold(oi * oi + ox * ox + oz * oz)

    def pass_one(i, d1):
        here, limit = n[i + 1], b[i + 1]
        di = clip(SIGMA * (n[i + 2] - here), limit)
        dx = clip(SIGMA * (ahead(here, 0) - here), limit)
        dz = clip(SIGMA * (ahead(here, 1) - here), limit)
        dual[0, i] = di
        dual[1, i] = dx
        dual[2, i] = dz
        div = di - step[...]
        div = div + (dx - behind(dx, 0))
        div = div + (dz - behind(dz, 1))
        step[...] = di
        v[i + 1] = here + (2.0 * GAIN) * div
        return d1 + squares(di, dx, dz)

    zero = jnp.zeros((8, 128), jnp.float32)

    def pass_group(k, d1):
        for copy in chunk(k, GROUP):
            copy.wait()
        for at in range(GROUP):
            d1 = pass_one(GROUP * k + at, d1)
        return d1

    early = min(EARLY, groups)
    loads[0].wait()
    d1 = lax.fori_loop(0, early, pass_group, zero)
    for k in range(1, 10):
        loads[k].wait()
    zc_up[0:1], zc_up[1:2], zc_up[2:3], zc_up[3:4] = nx_first[last], nx_last[last], bx_first[last], bx_last[last]
    zc_down[0:1], zc_down[1:2] = nx_first[first], nx_last[first]
    xc_up[0:1], xc_up[1:2], xc_up[2:3], xc_up[3:4] = nx_last[first], nx_last[last], bx_last[first], bx_last[last]
    xc_down[0:1], xc_down[1:2] = nx_first[first], nx_first[last]
    pl.semaphore_wait(barrier, greeted)
    got_zc_prev = send(zc_up, zc_prev, "inl", True)
    got_zc_next = send(zc_down, zc_next, "inl", False)
    got_xc_prev = send(xc_up, xc_prev, "xln", True)
    got_xc_next = send(xc_down, xc_next, "xln", False)
    got_n_prev = send(n.at[top], n.at[0], "inl", True)
    got_n_next = send(n.at[1], n.at[end], "inl", False)
    got_b_prev = send(b.at[top], b.at[0], "inl", True)
    got_nx_prev = send(nx_last, nx_prev, "xln", True)
    got_nx_next = send(nx_first, nx_next, "xln", False)
    got_bx_prev = send(bx_last, bx_prev, "xln", True)

    def edge(here, limit, side):
        di = clip(SIGMA * (ahead(here, 0) - here), limit)
        dz = clip(SIGMA * (ahead(here, 1) - here), limit)
        return here + (2.0 * GAIN) * ((di - behind(di, 0)) + side + (dz - behind(dz, 1)))

    inward = clip(SIGMA * (nx_second[...] - nx_first[...]), bx_first[...])
    vx_first[...] = edge(nx_first[...], bx_first[...], inward)
    inward = clip(SIGMA * (nx_last[...] - nx_semi[...]), bx_semi[...])
    vx_last[...] = edge(nx_last[...], bx_last[...], -inward)

    d1 = lax.fori_loop(early, groups, pass_group, d1)
    tail.wait()
    tail_n.wait()
    here, limit = n[top], b[top]
    dx = clip(SIGMA * (ahead(here, 0) - here), limit)
    dz = clip(SIGMA * (ahead(here, 1) - here), limit)
    dual[1, ni - 1] = dx
    dual[2, ni - 1] = dz
    div = (dx - behind(dx, 0)) - clip(SIGMA * (here - n[top - 1]), b[top - 1])
    div = div + (dz - behind(dz, 1))
    v[top] = here + (2.0 * GAIN) * div
    d1 = d1 + fold(dx * dx + dz * dz)
    for i in range(groups * GROUP, ni - 1):
        d1 = pass_one(i, d1)

    def no_prev(dst):
        def fill():
            dst[...] = jnp.zeros_like(dst)

        return fill

    def no_next(dst, low, high):
        def fill():
            dst[0:1] = low
            dst[1:2] = high

        return fill

    def grow(dst, rows, amount):
        dst[rows] = dst[rows] + (2.0 * GAIN) * amount

    got_zc_prev(no_prev(zc_prev))
    got_zc_next(no_next(zc_next, nx_first[last], nx_last[last]))
    grow(vx_first, first, -clip(SIGMA * (nx_first[first] - zc_prev[0:1]), zc_prev[2:3]))
    grow(vx_last, first, -clip(SIGMA * (nx_last[first] - zc_prev[1:2]), zc_prev[3:4]))
    grow(vx_first, last, clip(SIGMA * (zc_next[0:1] - nx_first[last]), bx_first[last]))
    grow(vx_last, last, clip(SIGMA * (zc_next[1:2] - nx_last[last]), bx_last[last]))
    got_vx_prev = send(vx_last, vx_prev, "xln", True)
    got_vx_next = send(vx_first, vx_next, "xln", False)
    got_xc_prev(no_prev(xc_prev))
    got_xc_next(no_next(xc_next, nx_last[first], nx_last[last]))
    for k, (rows, layer) in enumerate(((first, 1), (last, top))):
        outer = clip(SIGMA * (xc_next[k : k + 1] - nx_last[rows]), bx_last[rows])
        grow(v.at[layer], slice(nx - 1, nx), outer)
        outer = clip(SIGMA * (nx_first[rows] - xc_prev[k : k + 1]), xc_prev[2 + k : 3 + k])
        grow(v.at[layer], slice(0, 1), -outer)
    v_up = len(sent)
    got_v_prev = send(v.at[top], v.at[0], "inl", True)
    v_down = len(sent)
    got_v_next = send(v.at[1], v.at[end], "inl", False)

    if one_stage(ni_dev, nx_dev):
        for di in (2, -2):
            beyond = my_i - di // 2
            knows = jnp.logical_and(beyond >= 0, beyond < ni_dev)

            @pl.when(jnp.logical_and(knows, jnp.logical_and(my_i + di >= 0, my_i + di < ni_dev)))
            def _():
                pl.semaphore_signal(
                    far_sem, inc=1, device_id={"inl": my_i + di}, device_id_type=pl.DeviceIdType.MESH
                )

    row = lax.broadcasted_iota(jnp.int32, (8, nz), 0)

    def inner_rows(value, lo, hi):
        parts = split(value, 0, 8)
        if lo == 0:
            parts[0] = jnp.where(row == 0, 0.0, parts[0])
        if hi == nx:
            parts[-1] = jnp.where(row == 7, 0.0, parts[-1])
        return jnp.concatenate(parts, axis=0)

    def below(value, tile):
        turned = [pltpu.roll(part, 7, 0) for part in split(value, 0, 8)]
        over = [value[-8:] if tile is None else pltpu.roll(tile, 7, 0)]
        return jnp.concatenate([jnp.where(row == 7, x, t) for x, t in zip(turned[1:] + over, turned)], axis=0)

    def above(value, tile):
        turned = [pltpu.roll(part, 1, 0) for part in split(value, 0, 8)]
        under = [jnp.zeros_like(value[:8]) if tile is None else pltpu.roll(tile, 1, 0)]
        return jnp.concatenate([jnp.where(row == 0, x, t) for x, t in zip(under + turned[:-1], turned)], axis=0)

    def pass_two(i, so_far, lo=0, hi=nx, fresh=True):
        p1, p2, d2 = so_far
        here, limit, base = v[i + 1, lo:hi], b[i + 1, lo:hi], n[i + 1, lo:hi]
        oi, ox, oz = dual[0, i, lo:hi], dual[1, i, lo:hi], dual[2, i, lo:hi]
        di = clip(oi + SIGMA * (v[i + 2, lo:hi] - here), limit)
        dx = clip(ox + SIGMA * (below(here, v[i + 1, hi : hi + 8] if hi < nx else None) - here), limit)
        dz = clip(oz + SIGMA * (ahead(here, 1) - here), limit)
        if lo == 0:
            before = None
        elif fresh:
            before = v[i + 1, lo - 8 : lo]
            before = clip(dual[1, i, lo - 8 : lo] + SIGMA * (below(before, here[:8]) - before), b[i + 1, lo - 8 : lo])
        else:
            before = dual[1, i, lo - 8 : lo]
        dual[0, i, lo:hi] = di
        dual[1, i, lo:hi] = dx
        dual[2, i, lo:hi] = dz
        div = di - step[lo:hi]
        div = div + (dx - above(dx, before))
        div = div + (dz - behind(dz, 1))
        step[lo:hi] = di
        half = 0.5 * (here - base)
        change = GAIN * (div - half)
        out[i, lo:hi] = base + half + change
        inner = inner_rows(change, lo, hi)
        return (
            p1 + fold(half * half),
            p2 + fold(inner * inner),
            d2 + squares(di - oi, dx - ox, dz - oz),
        )

    def begin(lo, hi):
        step[lo:hi] = clip(
            dual[0, 1, lo:hi] + SIGMA * (v[3, lo:hi] - v[2, lo:hi]), b[2, lo:hi]
        )

    def middle(i, so_far):
        return pass_two(i, so_far, 8, nx - 8)

    def rim(i, so_far):
        return pass_two(i, pass_two(i, so_far, 0, 8), nx - 8, nx, False)

    begin(8, nx - 8)
    sums = stepped(2, ni - 2, middle, (zero,) * 3, MIDDLE)

    got_nx_prev(setter(nx_prev, nx_first))
    got_bx_prev(setter(bx_prev, bx_last))
    got_nx_next(setter(nx_next, nx_last))
    dx_last = clip(SIGMA * (nx_next[...] - nx_last[...]), bx_last[...])
    dxp = clip(SIGMA * (nx_first[...] - nx_prev[...]), bx_prev[...])
    dual[1, :, nx - 1, :] = dx_last
    dx_prev[...] = dxp
    dx_edge[...] = dx_last
    wx_last[...] = vx_last[...] + (2.0 * GAIN) * dx_last
    wx_first[...] = vx_first[...] - (2.0 * GAIN) * dxp
    v[2:top, nx - 1, :] = wx_last[1 : ni - 1]
    v[2:top, 0, :] = wx_first[1 : ni - 1]
    d1 = d1 + fold(dx_last * dx_last)

    begin(0, 8)
    begin(nx - 8, nx)
    sums = stepped(2, ni - 2, rim, sums, RIM)

    got_n_prev(setter(n.at[0], n.at[1]))
    got_b_prev(setter(b.at[0], b.at[1]))
    got_n_next(setter(n.at[end], n.at[top]))
    left(v_up)
    left(v_down)
    di_last = clip(SIGMA * (n[end] - n[top]), b[top])
    dip = clip(SIGMA * (n[1] - n[0]), b[0])
    dual[0, ni - 1] = di_last
    di_prev[...] = dip
    d1 = d1 + fold(di_last * di_last)
    v[top] = v[top] + (2.0 * GAIN) * di_last
    v[1] = v[1] - (2.0 * GAIN) * dip
    sums = pass_two(ni - 2, sums)
    step[...] = clip(dual[0, 0] + SIGMA * (v[2] - v[1]), b[1])
    sums = pass_two(1, sums)

    got_vx_prev(setter(vx_prev, wx_first))
    got_vx_next(setter(vx_next, wx_last))
    got_v_next(setter(v.at[end], v.at[top]))
    got_v_prev(setter(v.at[0], v.at[1]))
    v[end] = v[end] - (2.0 * GAIN) * dual[0, ni - 1]
    v[0] = v[0] + (2.0 * GAIN) * di_prev[...]
    step[...] = dual[0, ni - 2]
    sums = pass_two(ni - 1, sums)
    step[...] = clip(di_prev[...] + SIGMA * (v[1] - v[0]), b[0])
    p1, p2, d2 = pass_two(0, sums)

    was = dx_edge[...]
    dx_last = clip(
        was + SIGMA * (vx_next[...] - (2.0 * GAIN) * was - wx_last[...]), bx_last[...]
    )
    dual[1, :, nx - 1, :] = dx_last
    moved = dx_last - was
    d2 = d2 + fold(moved * moved)
    u_last = out[:, nx - 1, :] + GAIN * moved
    out[:, nx - 1, :] = u_last
    dxp = clip(
        dx_prev[...] + SIGMA * (wx_first[...] - (vx_prev[...] + (2.0 * GAIN) * dx_prev[...])), bx_prev[...]
    )
    u_first = out[:, 0, :] - GAIN * dxp
    out[:, 0, :] = u_first
    change = u_last - (nx_last[...] + 0.5 * (wx_last[...] - nx_last[...]))
    p2 = p2 + fold(change * change)
    change = u_first - (nx_first[...] + 0.5 * (wx_first[...] - nx_first[...]))
    p2 = p2 + fold(change * change)

    total = gather_lanes((p1, d1, p2, d2))
    if one_stage(ni_dev, nx_dev):
        far = 0
        for di in (3, -3):
            far = far + jnp.logical_and(my_i + di >= 0, my_i + di < ni_dev).astype(jnp.int32)
        if ni_dev > 3:
            @pl.when(far > 0)
            def _():
                pl.semaphore_wait(far_sem, 1)
    first = 0
    for stage, peers in enumerate(stages):
        mine[stage] = total
        for k, (di, dx) in enumerate(peers, first):
            pltpu.make_async_remote_copy(
                src_ref=mine.at[stage], dst_ref=others.at[k],
                send_sem=give_sem.at[stage], recv_sem=take_sem.at[stage],
                device_id=at(di, dx), device_id_type=pl.DeviceIdType.MESH,
            ).start()
        landed = others.at[pl.ds(first, len(peers))]
        if stage == 0:
            for slot in range(len(sent)):
                if slot not in (v_up, v_down):
                    left(slot)
        for sem in (give_sem, take_sem):
            pltpu.make_async_copy(landed, landed, sem.at[stage]).wait()
        rows = [total] + [others[k] for k in range(first, first + len(peers))]
        while len(rows) > 1:
            rows = [sum(rows[k + 1 : k + 2], rows[k]) for k in range(0, len(rows), 2)]
        total = rows[0]
        first += len(peers)
    norms[...] = jnp.sqrt(total[:, 0:2])


def put_out(out_held, dual_held, norms_held, out, dual, norms, sems):
    half = out.shape[0] // 2
    pairs = [(norms_held, norms)]
    for at in (0, half):
        part = pl.ds(at, half)
        pairs.append((out_held.at[part], out.at[part]))
        for axis in range(3):
            pairs.append((dual_held.at[axis, part], dual.at[axis, part]))
    copies = [pltpu.make_async_copy(src, dst, sems.at[k]) for k, (src, dst) in enumerate(pairs)]
    for copy in copies:
        copy.start()
    for copy in copies:
        copy.wait()


def per_device(noisy, bound):
    ni, nx, nz = noisy.shape
    ni_dev, nx_dev = lax.axis_size("inl"), lax.axis_size("xln")
    f32 = jnp.float32
    face = pltpu.VMEM((ni, nz), f32)
    slab = pltpu.VMEM((nx, nz), f32)
    dma = pltpu.SemaphoreType.DMA
    volume = 4 * ni * nx * nz
    stages = reduction(ni_dev, nx_dev)
    peers = sum(len(stage) for stage in stages)
    noisy = pltpu.with_memory_space_constraint(noisy, pltpu.HBM)
    bound = pltpu.with_memory_space_constraint(bound, pltpu.HBM)
    held = pl.pallas_call(
        functools.partial(kernel, ni_dev, nx_dev),
        out_shape=(
            pltpu.VMEM((ni, nx, nz), f32),
            pltpu.VMEM((3, ni, nx, nz), f32),
            pltpu.VMEM((2, 2), f32),
        ),
        in_specs=[pl.BlockSpec(memory_space=pltpu.HBM)] * 2,
        out_specs=(
            pl.BlockSpec(memory_space=pltpu.VMEM),
            pl.BlockSpec(memory_space=pltpu.VMEM),
            pl.BlockSpec(memory_space=pltpu.VMEM),
        ),
        scratch_shapes=[
            pltpu.VMEM((ni + 2, nx, nz), f32),
            pltpu.VMEM((ni + 1, nx, nz), f32),
            pltpu.VMEM((ni + 2, nx, nz), f32),
            slab,
            *([face] * 18),
            slab,
            *([pltpu.VMEM((4, nz), f32), pltpu.VMEM((2, nz), f32)] * 4),
            pltpu.VMEM((len(stages), 2, 128), f32),
            pltpu.VMEM((peers, 2, 128), f32),
            dma((10,)), dma((2, (ni - 1) // GROUP + 1)), dma((14,)), dma((14,)), dma((len(stages),)), dma((len(stages),)),
            pltpu.SemaphoreType.REGULAR,
        ],
        compiler_params=pltpu.CompilerParams(
            collective_id=0, has_side_effects=True, vmem_limit_bytes=24 * 1024 * 1024
        ),
        cost_estimate=pl.CostEstimate(
            flops=80 * ni * nx * nz, bytes_accessed=6 * volume, transcendentals=0
        ),
        name="denoise",
    )(noisy, bound)
    in_vmem = pl.BlockSpec(memory_space=pltpu.VMEM)
    in_hbm = pl.BlockSpec(memory_space=pltpu.HBM)
    return pl.pallas_call(
        put_out,
        out_shape=(
            jax.ShapeDtypeStruct((ni, nx, nz), f32),
            jax.ShapeDtypeStruct((3, ni, nx, nz), f32),
            jax.ShapeDtypeStruct((2, 2), f32),
        ),
        in_specs=[in_vmem] * 3,
        out_specs=(in_hbm,) * 3,
        scratch_shapes=[dma((9,))],
        compiler_params=pltpu.CompilerParams(vmem_limit_bytes=1024 * 1024),
        cost_estimate=pl.CostEstimate(flops=0, bytes_accessed=4 * volume, transcendentals=0),
        name="put_out",
    )(*held)


def solution(mesh):
    in_specs = (P("inl", "xln", None), P("inl", "xln", None))
    out_specs = (P("inl", "xln", None), P(None, "inl", "xln", None), P())
    return jax.shard_map(
        per_device, mesh=mesh, in_specs=in_specs, out_specs=out_specs, check_vma=False
    )
```

```python
import functools

import jax
import jax.numpy as jnp
from jax import lax
from jax.experimental import pallas as pl
from jax.experimental.pallas import tpu as pltpu
from jax.sharding import PartitionSpec as P

SIGMA = 0.28
TAU = 0.28
GAIN = TAU / (1.0 + TAU)
GROUP = 4
AHEAD = 1
EARLY = 1
MIDDLE = 7
RIM = 7


def clip(value, limit):
    return jnp.minimum(jnp.maximum(value, -limit), limit)


def fold(square):
    rows, lanes = square.shape
    total = square[0:8]
    for at in range(8, rows, 8):
        total = total + square[at : at + 8]
    part = total[:, 0:128]
    for at in range(128, lanes, 128):
        part = part + total[:, at : at + 128]
    return part


def gather_lanes(parts):
    lane = lax.broadcasted_iota(jnp.int32, (2, 128), 1)
    row = lax.broadcasted_iota(jnp.int32, (2, 128), 0)
    result = jnp.zeros((2, 128), jnp.float32)
    for k, part in enumerate(parts):
        total = jnp.sum(jnp.sum(part, axis=0, keepdims=True), axis=1, keepdims=True)
        result = jnp.where(jnp.logical_and(row == k // 2, lane == k % 2), total, result)
    return result


def one_stage(ni_dev, nx_dev):
    return ni_dev <= 4 and ni_dev * nx_dev <= 32


def reduction(ni_dev, nx_dev):
    around = [[*range(1, count), 0] for count in (ni_dev, nx_dev)]
    everyone = [(di, dx) for di in around[0] for dx in around[1] if di or dx]
    if one_stage(ni_dev, nx_dev):
        return [everyone]
    return [[peer for peer in everyone if peer[0] == 0], [peer for peer in everyone if peer[1] == 0]]


def stepped(start, stop, body, carry, unroll=4):
    def group(k, carry):
        for at in range(unroll):
            carry = body(start + k * unroll + at, carry)
        return carry

    whole = (stop - start) // unroll
    carry = lax.fori_loop(0, whole, group, carry)
    for i in range(start + whole * unroll, stop):
        carry = body(i, carry)
    return carry


def split(value, dim, size):
    return [lax.slice_in_dim(value, at, at + size, axis=dim) for at in range(0, value.shape[dim], size)]


def ahead(value, dim):
    size = (8, 128)[dim]
    parts = split(value, dim, size)
    turned = [pltpu.roll(part, size - 1, dim) for part in parts]
    edge = lax.broadcasted_iota(jnp.int32, parts[0].shape, dim) == size - 1
    after = turned[1:] + [parts[-1]]
    return jnp.concatenate([jnp.where(edge, a, t) for a, t in zip(after, turned)], axis=dim)


def behind(value, dim):
    size = (8, 128)[dim]
    turned = [pltpu.roll(part, 1, dim) for part in split(value, dim, size)]
    edge = lax.broadcasted_iota(jnp.int32, turned[0].shape, dim) == 0
    before = [jnp.zeros_like(turned[0])] + turned[:-1]
    return jnp.concatenate([jnp.where(edge, a, t) for a, t in zip(before, turned)], axis=dim)


def kernel(
    ni_dev, nx_dev,
    noisy, bound, out, dual, norms,
    n, b, v, step,
    nx_first, nx_last, bx_last, bx_first, nx_second, nx_semi, bx_semi,
    nx_next, nx_prev, bx_prev,
    vx_first, vx_last, vx_next, vx_prev, wx_first, wx_last, dx_prev, dx_edge, di_prev,
    zc_up, zc_down, zc_prev, zc_next, xc_up, xc_down, xc_prev, xc_next,
    mine, others,
    load_sem, chunk_sem, send_sem, recv_sem, give_sem, take_sem, far_sem,
):
    ni, nx, nz = noisy.shape
    top, end = ni, ni + 1
    my_i, my_x = lax.axis_index("inl"), lax.axis_index("xln")
    f32 = jnp.float32

    barrier = pltpu.get_barrier_semaphore()
    stages = reduction(ni_dev, nx_dev)

    def at(di, dx):
        return {"inl": lax.rem(my_i + di, ni_dev), "xln": lax.rem(my_x + dx, nx_dev)}

    loads = []

    def load(src, dst):
        copy = pltpu.make_async_copy(src, dst, load_sem.at[len(loads)])
        copy.start()
        loads.append(copy)

    def chunk(k, size):
        return (
            pltpu.make_async_copy(
                noisy.at[pl.ds(GROUP * k + 1, size)], n.at[pl.ds(GROUP * k + 2, size)], chunk_sem.at[0, k]
            ),
            pltpu.make_async_copy(
                bound.at[pl.ds(GROUP * k, size)], b.at[pl.ds(GROUP * k + 1, size)], chunk_sem.at[1, k]
            ),
        )

    groups = (ni - 1) // GROUP
    rest = ni - 1 - groups * GROUP
    pieces = [(k, GROUP) for k in range(groups)]
    tail = pltpu.make_async_copy(
        bound.at[pl.ds(ni - 1 - rest, rest)], b.at[pl.ds(ni - rest, rest)], chunk_sem.at[1, groups]
    )
    tail_n = pltpu.make_async_copy(
        noisy.at[pl.ds(ni - rest, rest - 1)], n.at[pl.ds(ni - rest + 1, rest - 1)], chunk_sem.at[0, groups]
    )
    load(noisy.at[pl.ds(0, 1)], n.at[pl.ds(1, 1)])
    for k, size in pieces[:AHEAD]:
        for copy in chunk(k, size):
            copy.start()
    hello = [(di, 0) for di in range(1 - ni_dev, ni_dev) if di and (abs(di) == 1 or not one_stage(ni_dev, nx_dev))]
    hello = sorted(hello, key=lambda peer: abs(peer[0])) + [(0, dx) for dx in range(1, nx_dev)]
    greeted = 0
    for di, dx in hello:
        exists = jnp.logical_and(my_i + di >= 0, my_i + di < ni_dev)
        greeted = greeted + exists.astype(jnp.int32)

        @pl.when(exists)
        def _():
            pl.semaphore_signal(
                barrier, inc=1,
                device_id={"inl": my_i + di, "xln": lax.rem(my_x + dx, nx_dev)},
                device_id_type=pl.DeviceIdType.MESH,
            )

    load(noisy.at[:, 0, :], nx_first)
    load(noisy.at[:, nx - 1, :], nx_last)
    load(bound.at[:, nx - 1, :], bx_last)
    load(bound.at[:, 0, :], bx_first)
    load(noisy.at[pl.ds(ni - 1, 1)], n.at[pl.ds(top, 1)])
    load(bound.at[pl.ds(ni - 1, 1)], b.at[pl.ds(top, 1)])
    load(noisy.at[:, 1, :], nx_second)
    load(noisy.at[:, nx - 2, :], nx_semi)
    load(bound.at[:, nx - 2, :], bx_semi)
    for k, size in pieces[AHEAD:]:
        for copy in chunk(k, size):
            copy.start()
    tail.start()
    tail_n.start()

    sent = []

    def send(src, dst, axis, forward):
        slot = len(sent)
        me, count = (my_i, ni_dev) if axis == "inl" else (my_x, nx_dev)
        target = lax.rem(me + (1 if forward else count - 1), count)
        copy = pltpu.make_async_remote_copy(
            src_ref=src, dst_ref=dst, send_sem=send_sem.at[slot], recv_sem=recv_sem.at[slot],
            device_id={axis: target}, device_id_type=pl.DeviceIdType.MESH,
        )
        not_last, not_first = me < count - 1, me > 0
        can_send, can_recv = (not_last, not_first) if forward else (not_first, not_last)

        @pl.when(can_send)
        def _():
            copy.start()

        sent.append((copy, can_send))

        def arrive(fill):
            @pl.when(can_recv)
            def _():
                copy.wait_recv()

            @pl.when(jnp.logical_not(can_recv))
            def _():
                fill()

        return arrive

    def left(slot):
        copy, can_send = sent[slot]

        @pl.when(can_send)
        def _():
            copy.wait_send()

    def setter(dst, src):
        def fill():
            dst[...] = src[...]

        return fill

    first, last = slice(0, 1), slice(ni - 1, ni)

    step[...] = jnp.zeros_like(step)

    def squares(oi, ox, oz):
        return fold(oi * oi + ox * ox + oz * oz)

    def pass_one(i, d1):
        here, limit = n[i + 1], b[i + 1]
        scaled = SIGMA * here
        di = clip(SIGMA * n[i + 2] - scaled, limit)
        dx = clip(ahead(scaled, 0) - scaled, limit)
        dz = clip(ahead(scaled, 1) - scaled, limit)
        dual[0, i] = di
        dual[1, i] = dx
        dual[2, i] = dz
        div = di - step[...]
        div = div + (dx - behind(dx, 0))
        div = div + (dz - behind(dz, 1))
        step[...] = di
        v[i + 1] = here + (2.0 * GAIN) * div
        return d1 + squares(di, dx, dz)

    zero = jnp.zeros((8, 128), jnp.float32)

    def pass_group(k, d1):
        for copy in chunk(k, GROUP):
            copy.wait()
        for at in range(GROUP):
            d1 = pass_one(GROUP * k + at, d1)
        return d1

    early = min(EARLY, groups)
    loads[0].wait()
    d1 = lax.fori_loop(0, early, pass_group, zero)
    for k in range(1, 10):
        loads[k].wait()
    zc_up[0:1], zc_up[1:2], zc_up[2:3], zc_up[3:4] = nx_first[last], nx_last[last], bx_first[last], bx_last[last]
    zc_down[0:1], zc_down[1:2] = nx_first[first], nx_last[first]
    xc_up[0:1], xc_up[1:2], xc_up[2:3], xc_up[3:4] = nx_last[first], nx_last[last], bx_last[first], bx_last[last]
    xc_down[0:1], xc_down[1:2] = nx_first[first], nx_first[last]
    pl.semaphore_wait(barrier, greeted)
    got_zc_prev = send(zc_up, zc_prev, "inl", True)
    got_zc_next = send(zc_down, zc_next, "inl", False)
    got_xc_prev = send(xc_up, xc_prev, "xln", True)
    got_xc_next = send(xc_down, xc_next, "xln", False)
    got_n_prev = send(n.at[top], n.at[0], "inl", True)
    got_n_next = send(n.at[1], n.at[end], "inl", False)
    got_b_prev = send(b.at[top], b.at[0], "inl", True)
    got_nx_prev = send(nx_last, nx_prev, "xln", True)
    got_nx_next = send(nx_first, nx_next, "xln", False)
    got_bx_prev = send(bx_last, bx_prev, "xln", True)

    def edge(here, limit, side):
        di = clip(SIGMA * (ahead(here, 0) - here), limit)
        dz = clip(SIGMA * (ahead(here, 1) - here), limit)
        return here + (2.0 * GAIN) * ((di - behind(di, 0)) + side + (dz - behind(dz, 1)))

    inward = clip(SIGMA * (nx_second[...] - nx_first[...]), bx_first[...])
    vx_first[...] = edge(nx_first[...], bx_first[...], inward)
    inward = clip(SIGMA * (nx_last[...] - nx_semi[...]), bx_semi[...])
    vx_last[...] = edge(nx_last[...], bx_last[...], -inward)

    d1 = lax.fori_loop(early, groups, pass_group, d1)
    tail.wait()
    tail_n.wait()
    here, limit = n[top], b[top]
    dx = clip(SIGMA * (ahead(here, 0) - here), limit)
    dz = clip(SIGMA * (ahead(here, 1) - here), limit)
    dual[1, ni - 1] = dx
    dual[2, ni - 1] = dz
    div = (dx - behind(dx, 0)) - clip(SIGMA * (here - n[top - 1]), b[top - 1])
    div = div + (dz - behind(dz, 1))
    v[top] = here + (2.0 * GAIN) * div
    d1 = d1 + fold(dx * dx + dz * dz)
    for i in range(groups * GROUP, ni - 1):
        d1 = pass_one(i, d1)

    def no_prev(dst):
        def fill():
            dst[...] = jnp.zeros_like(dst)

        return fill

    def no_next(dst, low, high):
        def fill():
            dst[0:1] = low
            dst[1:2] = high

        return fill

    def grow(dst, rows, amount):
        dst[rows] = dst[rows] + (2.0 * GAIN) * amount

    got_zc_prev(no_prev(zc_prev))
    got_zc_next(no_next(zc_next, nx_first[last], nx_last[last]))
    grow(vx_first, first, -clip(SIGMA * (nx_first[first] - zc_prev[0:1]), zc_prev[2:3]))
    grow(vx_last, first, -clip(SIGMA * (nx_last[first] - zc_prev[1:2]), zc_prev[3:4]))
    grow(vx_first, last, clip(SIGMA * (zc_next[0:1] - nx_first[last]), bx_first[last]))
    grow(vx_last, last, clip(SIGMA * (zc_next[1:2] - nx_last[last]), bx_last[last]))
    got_vx_prev = send(vx_last, vx_prev, "xln", True)
    got_vx_next = send(vx_first, vx_next, "xln", False)
    got_xc_prev(no_prev(xc_prev))
    got_xc_next(no_next(xc_next, nx_last[first], nx_last[last]))
    for k, (rows, layer) in enumerate(((first, 1), (last, top))):
        outer = clip(SIGMA * (xc_next[k : k + 1] - nx_last[rows]), bx_last[rows])
        grow(v.at[layer], slice(nx - 1, nx), outer)
        outer = clip(SIGMA * (nx_first[rows] - xc_prev[k : k + 1]), xc_prev[2 + k : 3 + k])
        grow(v.at[layer], slice(0, 1), -outer)
    v_up = len(sent)
    got_v_prev = send(v.at[top], v.at[0], "inl", True)
    v_down = len(sent)
    got_v_next = send(v.at[1], v.at[end], "inl", False)

    if one_stage(ni_dev, nx_dev):
        for di in (2, -2):
            beyond = my_i - di // 2
            knows = jnp.logical_and(beyond >= 0, beyond < ni_dev)

            @pl.when(jnp.logical_and(knows, jnp.logical_and(my_i + di >= 0, my_i + di < ni_dev)))
            def _():
                pl.semaphore_signal(
                    far_sem, inc=1, device_id={"inl": my_i + di}, device_id_type=pl.DeviceIdType.MESH
                )

    row = lax.broadcasted_iota(jnp.int32, (8, nz), 0)

    def inner_rows(value, lo, hi):
        parts = split(value, 0, 8)
        if lo == 0:
            parts[0] = jnp.where(row == 0, 0.0, parts[0])
        if hi == nx:
            parts[-1] = jnp.where(row == 7, 0.0, parts[-1])
        return jnp.concatenate(parts, axis=0)

    def below(value, tile):
        turned = [pltpu.roll(part, 7, 0) for part in split(value, 0, 8)]
        over = [value[-8:] if tile is None else pltpu.roll(tile, 7, 0)]
        return jnp.concatenate([jnp.where(row == 7, x, t) for x, t in zip(turned[1:] + over, turned)], axis=0)

    def above(value, tile):
        turned = [pltpu.roll(part, 1, 0) for part in split(value, 0, 8)]
        under = [jnp.zeros_like(value[:8]) if tile is None else pltpu.roll(tile, 1, 0)]
        return jnp.concatenate([jnp.where(row == 0, x, t) for x, t in zip(under + turned[:-1], turned)], axis=0)

    def pass_two(i, so_far, lo=0, hi=nx, fresh=True):
        p1, p2, d2 = so_far
        here, limit, base = v[i + 1, lo:hi], b[i + 1, lo:hi], n[i + 1, lo:hi]
        oi, ox, oz = dual[0, i, lo:hi], dual[1, i, lo:hi], dual[2, i, lo:hi]
        scaled = SIGMA * here
        di = clip(oi + (SIGMA * v[i + 2, lo:hi] - scaled), limit)
        dx = clip(ox + (below(scaled, SIGMA * v[i + 1, hi : hi + 8] if hi < nx else None) - scaled), limit)
        dz = clip(oz + (ahead(scaled, 1) - scaled), limit)
        if lo == 0:
            before = None
        elif fresh:
            before = v[i + 1, lo - 8 : lo]
            before = clip(dual[1, i, lo - 8 : lo] + SIGMA * (below(before, here[:8]) - before), b[i + 1, lo - 8 : lo])
        else:
            before = dual[1, i, lo - 8 : lo]
        dual[0, i, lo:hi] = di
        dual[1, i, lo:hi] = dx
        dual[2, i, lo:hi] = dz
        div = di - step[lo:hi]
        div = div + (dx - above(dx, before))
        div = div + (dz - behind(dz, 1))
        step[lo:hi] = di
        half = 0.5 * (here - base)
        change = GAIN * (div - half)
        out[i, lo:hi] = base + half + change
        inner = inner_rows(change, lo, hi)
        return (
            p1 + fold(half * half),
            p2 + fold(inner * inner),
            d2 + squares(di - oi, dx - ox, dz - oz),
        )

    def begin(lo, hi):
        step[lo:hi] = clip(
            dual[0, 1, lo:hi] + SIGMA * (v[3, lo:hi] - v[2, lo:hi]), b[2, lo:hi]
        )

    def middle(i, so_far):
        return pass_two(i, so_far, 8, nx - 8)

    def rim(i, so_far):
        return pass_two(i, pass_two(i, so_far, 0, 8), nx - 8, nx, False)

    begin(8, nx - 8)
    sums = stepped(2, ni - 2, middle, (zero,) * 3, MIDDLE)

    got_nx_prev(setter(nx_prev, nx_first))
    got_bx_prev(setter(bx_prev, bx_last))
    got_nx_next(setter(nx_next, nx_last))
    dx_last = clip(SIGMA * (nx_next[...] - nx_last[...]), bx_last[...])
    dxp = clip(SIGMA * (nx_first[...] - nx_prev[...]), bx_prev[...])
    dual[1, :, nx - 1, :] = dx_last
    dx_prev[...] = dxp
    dx_edge[...] = dx_last
    wx_last[...] = vx_last[...] + (2.0 * GAIN) * dx_last
    wx_first[...] = vx_first[...] - (2.0 * GAIN) * dxp
    v[2:top, nx - 1, :] = wx_last[1 : ni - 1]
    v[2:top, 0, :] = wx_first[1 : ni - 1]
    d1 = d1 + fold(dx_last * dx_last)

    begin(0, 8)
    begin(nx - 8, nx)
    sums = stepped(2, ni - 2, rim, sums, RIM)

    got_n_prev(setter(n.at[0], n.at[1]))
    got_b_prev(setter(b.at[0], b.at[1]))
    got_n_next(setter(n.at[end], n.at[top]))
    left(v_up)
    left(v_down)
    di_last = clip(SIGMA * (n[end] - n[top]), b[top])
    dip = clip(SIGMA * (n[1] - n[0]), b[0])
    dual[0, ni - 1] = di_last
    di_prev[...] = dip
    d1 = d1 + fold(di_last * di_last)
    v[top] = v[top] + (2.0 * GAIN) * di_last
    v[1] = v[1] - (2.0 * GAIN) * dip
    sums = pass_two(ni - 2, sums)
    step[...] = clip(dual[0, 0] + SIGMA * (v[2] - v[1]), b[1])
    sums = pass_two(1, sums)

    got_vx_prev(setter(vx_prev, wx_first))
    got_vx_next(setter(vx_next, wx_last))
    got_v_next(setter(v.at[end], v.at[top]))
    got_v_prev(setter(v.at[0], v.at[1]))
    v[end] = v[end] - (2.0 * GAIN) * dual[0, ni - 1]
    v[0] = v[0] + (2.0 * GAIN) * di_prev[...]
    step[...] = dual[0, ni - 2]
    sums = pass_two(ni - 1, sums)
    step[...] = clip(di_prev[...] + SIGMA * (v[1] - v[0]), b[0])
    p1, p2, d2 = pass_two(0, sums)

    was = dx_edge[...]
    dx_last = clip(
        was + SIGMA * (vx_next[...] - (2.0 * GAIN) * was - wx_last[...]), bx_last[...]
    )
    dual[1, :, nx - 1, :] = dx_last
    moved = dx_last - was
    d2 = d2 + fold(moved * moved)
    u_last = out[:, nx - 1, :] + GAIN * moved
    out[:, nx - 1, :] = u_last
    dxp = clip(
        dx_prev[...] + SIGMA * (wx_first[...] - (vx_prev[...] + (2.0 * GAIN) * dx_prev[...])), bx_prev[...]
    )
    u_first = out[:, 0, :] - GAIN * dxp
    out[:, 0, :] = u_first
    change = u_last - (nx_last[...] + 0.5 * (wx_last[...] - nx_last[...]))
    p2 = p2 + fold(change * change)
    change = u_first - (nx_first[...] + 0.5 * (wx_first[...] - nx_first[...]))
    p2 = p2 + fold(change * change)

    total = gather_lanes((p1, d1, p2, d2))
    if one_stage(ni_dev, nx_dev):
        far = 0
        for di in (3, -3):
            far = far + jnp.logical_and(my_i + di >= 0, my_i + di < ni_dev).astype(jnp.int32)
        if ni_dev > 3:
            @pl.when(far > 0)
            def _():
                pl.semaphore_wait(far_sem, 1)
    first = 0
    for stage, peers in enumerate(stages):
        mine[stage] = total
        for k, (di, dx) in enumerate(peers, first):
            pltpu.make_async_remote_copy(
                src_ref=mine.at[stage], dst_ref=others.at[k],
                send_sem=give_sem.at[stage], recv_sem=take_sem.at[stage],
                device_id=at(di, dx), device_id_type=pl.DeviceIdType.MESH,
            ).start()
        landed = others.at[pl.ds(first, len(peers))]
        if stage == 0:
            for slot in range(len(sent)):
                if slot not in (v_up, v_down):
                    left(slot)
        for sem in (give_sem, take_sem):
            pltpu.make_async_copy(landed, landed, sem.at[stage]).wait()
        rows = [total] + [others[k] for k in range(first, first + len(peers))]
        while len(rows) > 1:
            rows = [sum(rows[k + 1 : k + 2], rows[k]) for k in range(0, len(rows), 2)]
        total = rows[0]
        first += len(peers)
    norms[...] = jnp.sqrt(total[:, 0:2])


def put_out(out_held, dual_held, norms_held, out, dual, norms, sems):
    half = out.shape[0] // 2
    pairs = [(norms_held, norms)]
    for at in (0, half):
        part = pl.ds(at, half)
        pairs.append((out_held.at[part], out.at[part]))
        for axis in range(3):
            pairs.append((dual_held.at[axis, part], dual.at[axis, part]))
    copies = [pltpu.make_async_copy(src, dst, sems.at[k]) for k, (src, dst) in enumerate(pairs)]
    for copy in copies:
        copy.start()
    for copy in copies:
        copy.wait()


def per_device(noisy, bound):
    ni, nx, nz = noisy.shape
    ni_dev, nx_dev = lax.axis_size("inl"), lax.axis_size("xln")
    f32 = jnp.float32
    face = pltpu.VMEM((ni, nz), f32)
    slab = pltpu.VMEM((nx, nz), f32)
    dma = pltpu.SemaphoreType.DMA
    volume = 4 * ni * nx * nz
    stages = reduction(ni_dev, nx_dev)
    peers = sum(len(stage) for stage in stages)
    noisy = pltpu.with_memory_space_constraint(noisy, pltpu.HBM)
    bound = pltpu.with_memory_space_constraint(bound, pltpu.HBM)
    held = pl.pallas_call(
        functools.partial(kernel, ni_dev, nx_dev),
        out_shape=(
            pltpu.VMEM((ni, nx, nz), f32),
            pltpu.VMEM((3, ni, nx, nz), f32),
            pltpu.VMEM((2, 2), f32),
        ),
        in_specs=[pl.BlockSpec(memory_space=pltpu.HBM)] * 2,
        out_specs=(
            pl.BlockSpec(memory_space=pltpu.VMEM),
            pl.BlockSpec(memory_space=pltpu.VMEM),
            pl.BlockSpec(memory_space=pltpu.VMEM),
        ),
        scratch_shapes=[
            pltpu.VMEM((ni + 2, nx, nz), f32),
            pltpu.VMEM((ni + 1, nx, nz), f32),
            pltpu.VMEM((ni + 2, nx, nz), f32),
            slab,
            *([face] * 18),
            slab,
            *([pltpu.VMEM((4, nz), f32), pltpu.VMEM((2, nz), f32)] * 4),
            pltpu.VMEM((len(stages), 2, 128), f32),
            pltpu.VMEM((peers, 2, 128), f32),
            dma((10,)), dma((2, (ni - 1) // GROUP + 1)), dma((14,)), dma((14,)), dma((len(stages),)), dma((len(stages),)),
            pltpu.SemaphoreType.REGULAR,
        ],
        compiler_params=pltpu.CompilerParams(
            collective_id=0, has_side_effects=True, vmem_limit_bytes=24 * 1024 * 1024
        ),
        cost_estimate=pl.CostEstimate(
            flops=80 * ni * nx * nz, bytes_accessed=6 * volume, transcendentals=0
        ),
        name="denoise",
    )(noisy, bound)
    in_vmem = pl.BlockSpec(memory_space=pltpu.VMEM)
    in_hbm = pl.BlockSpec(memory_space=pltpu.HBM)
    return pl.pallas_call(
        put_out,
        out_shape=(
            jax.ShapeDtypeStruct((ni, nx, nz), f32),
            jax.ShapeDtypeStruct((3, ni, nx, nz), f32),
            jax.ShapeDtypeStruct((2, 2), f32),
        ),
        in_specs=[in_vmem] * 3,
        out_specs=(in_hbm,) * 3,
        scratch_shapes=[dma((9,))],
        compiler_params=pltpu.CompilerParams(vmem_limit_bytes=1024 * 1024),
        cost_estimate=pl.CostEstimate(flops=0, bytes_accessed=4 * volume, transcendentals=0),
        name="put_out",
    )(*held)


def solution(mesh):
    in_specs = (P("inl", "xln", None), P("inl", "xln", None))
    out_specs = (P("inl", "xln", None), P(None, "inl", "xln", None), P())
    return jax.shard_map(
        per_device, mesh=mesh, in_specs=in_specs, out_specs=out_specs, check_vma=False
    )
```

```python
import functools

import jax
import jax.numpy as jnp
from jax import lax
from jax.experimental import pallas as pl
from jax.experimental.pallas import tpu as pltpu
from jax.sharding import PartitionSpec as P

SIGMA = 0.28
TAU = 0.28
GAIN = TAU / (1.0 + TAU)
GROUP = 4
AHEAD = 1
EARLY = 1
MIDDLE = 14
RIM = 7


def clip(value, limit):
    return jnp.minimum(jnp.maximum(value, -limit), limit)


def fold(square):
    rows, lanes = square.shape
    total = square[0:8]
    for at in range(8, rows, 8):
        total = total + square[at : at + 8]
    part = total[:, 0:128]
    for at in range(128, lanes, 128):
        part = part + total[:, at : at + 128]
    return part


def gather_lanes(parts):
    lane = lax.broadcasted_iota(jnp.int32, (2, 128), 1)
    row = lax.broadcasted_iota(jnp.int32, (2, 128), 0)
    result = jnp.zeros((2, 128), jnp.float32)
    for k, part in enumerate(parts):
        total = jnp.sum(jnp.sum(part, axis=0, keepdims=True), axis=1, keepdims=True)
        result = jnp.where(jnp.logical_and(row == k // 2, lane == k % 2), total, result)
    return result


def one_stage(ni_dev, nx_dev):
    return ni_dev <= 4 and ni_dev * nx_dev <= 32


def reduction(ni_dev, nx_dev):
    around = [[*range(1, count), 0] for count in (ni_dev, nx_dev)]
    everyone = [(di, dx) for di in around[0] for dx in around[1] if di or dx]
    if one_stage(ni_dev, nx_dev):
        return [everyone]
    return [[peer for peer in everyone if peer[0] == 0], [peer for peer in everyone if peer[1] == 0]]


def stepped(start, stop, body, carry, unroll=4):
    def group(k, carry):
        for at in range(unroll):
            carry = body(start + k * unroll + at, carry)
        return carry

    whole = (stop - start) // unroll
    carry = lax.fori_loop(0, whole, group, carry)
    for i in range(start + whole * unroll, stop):
        carry = body(i, carry)
    return carry


def split(value, dim, size):
    return [lax.slice_in_dim(value, at, at + size, axis=dim) for at in range(0, value.shape[dim], size)]


def ahead(value, dim):
    size = (8, 128)[dim]
    parts = split(value, dim, size)
    turned = [pltpu.roll(part, size - 1, dim) for part in parts]
    edge = lax.broadcasted_iota(jnp.int32, parts[0].shape, dim) == size - 1
    after = turned[1:] + [parts[-1]]
    return jnp.concatenate([jnp.where(edge, a, t) for a, t in zip(after, turned)], axis=dim)


def behind(value, dim):
    size = (8, 128)[dim]
    turned = [pltpu.roll(part, 1, dim) for part in split(value, dim, size)]
    edge = lax.broadcasted_iota(jnp.int32, turned[0].shape, dim) == 0
    before = [jnp.zeros_like(turned[0])] + turned[:-1]
    return jnp.concatenate([jnp.where(edge, a, t) for a, t in zip(before, turned)], axis=dim)


def kernel(
    ni_dev, nx_dev,
    noisy, bound, out, dual, norms,
    n, b, v, step,
    nx_first, nx_last, bx_last, bx_first, nx_second, nx_semi, bx_semi,
    nx_next, nx_prev, bx_prev,
    vx_first, vx_last, vx_next, vx_prev, wx_first, wx_last, dx_prev, dx_edge, di_prev,
    zc_up, zc_down, zc_prev, zc_next, xc_up, xc_down, xc_prev, xc_next,
    mine, others,
    load_sem, chunk_sem, send_sem, recv_sem, give_sem, take_sem, far_sem,
):
    ni, nx, nz = noisy.shape
    top, end = ni, ni + 1
    my_i, my_x = lax.axis_index("inl"), lax.axis_index("xln")
    f32 = jnp.float32

    barrier = pltpu.get_barrier_semaphore()
    stages = reduction(ni_dev, nx_dev)

    def at(di, dx):
        return {"inl": lax.rem(my_i + di, ni_dev), "xln": lax.rem(my_x + dx, nx_dev)}

    loads = []

    def load(src, dst):
        copy = pltpu.make_async_copy(src, dst, load_sem.at[len(loads)])
        copy.start()
        loads.append(copy)

    def chunk(k, size):
        return (
            pltpu.make_async_copy(
                noisy.at[pl.ds(GROUP * k + 1, size)], n.at[pl.ds(GROUP * k + 2, size)], chunk_sem.at[0, k]
            ),
            pltpu.make_async_copy(
                bound.at[pl.ds(GROUP * k, size)], b.at[pl.ds(GROUP * k + 1, size)], chunk_sem.at[1, k]
            ),
        )

    groups = (ni - 1) // GROUP
    rest = ni - 1 - groups * GROUP
    pieces = [(k, GROUP) for k in range(groups)]
    tail = pltpu.make_async_copy(
        bound.at[pl.ds(ni - 1 - rest, rest)], b.at[pl.ds(ni - rest, rest)], chunk_sem.at[1, groups]
    )
    tail_n = pltpu.make_async_copy(
        noisy.at[pl.ds(ni - rest, rest - 1)], n.at[pl.ds(ni - rest + 1, rest - 1)], chunk_sem.at[0, groups]
    )
    load(noisy.at[pl.ds(0, 1)], n.at[pl.ds(1, 1)])
    for k, size in pieces[:AHEAD]:
        for copy in chunk(k, size):
            copy.start()
    hello = [(di, 0) for di in range(1 - ni_dev, ni_dev) if di and (abs(di) == 1 or not one_stage(ni_dev, nx_dev))]
    hello = sorted(hello, key=lambda peer: abs(peer[0])) + [(0, dx) for dx in range(1, nx_dev)]
    greeted = 0
    for di, dx in hello:
        exists = jnp.logical_and(my_i + di >= 0, my_i + di < ni_dev)
        greeted = greeted + exists.astype(jnp.int32)

        @pl.when(exists)
        def _():
            pl.semaphore_signal(
                barrier, inc=1,
                device_id={"inl": my_i + di, "xln": lax.rem(my_x + dx, nx_dev)},
                device_id_type=pl.DeviceIdType.MESH,
            )

    load(noisy.at[:, 0, :], nx_first)
    load(noisy.at[:, nx - 1, :], nx_last)
    load(bound.at[:, nx - 1, :], bx_last)
    load(bound.at[:, 0, :], bx_first)
    load(noisy.at[pl.ds(ni - 1, 1)], n.at[pl.ds(top, 1)])
    load(bound.at[pl.ds(ni - 1, 1)], b.at[pl.ds(top, 1)])
    load(noisy.at[:, 1, :], nx_second)
    load(noisy.at[:, nx - 2, :], nx_semi)
    load(bound.at[:, nx - 2, :], bx_semi)
    for k, size in pieces[AHEAD:]:
        for copy in chunk(k, size):
            copy.start()
    tail.start()
    tail_n.start()

    sent = []

    def send(src, dst, axis, forward):
        slot = len(sent)
        me, count = (my_i, ni_dev) if axis == "inl" else (my_x, nx_dev)
        target = lax.rem(me + (1 if forward else count - 1), count)
        copy = pltpu.make_async_remote_copy(
            src_ref=src, dst_ref=dst, send_sem=send_sem.at[slot], recv_sem=recv_sem.at[slot],
            device_id={axis: target}, device_id_type=pl.DeviceIdType.MESH,
        )
        not_last, not_first = me < count - 1, me > 0
        can_send, can_recv = (not_last, not_first) if forward else (not_first, not_last)

        @pl.when(can_send)
        def _():
            copy.start()

        sent.append((copy, can_send))

        def arrive(fill):
            @pl.when(can_recv)
            def _():
                copy.wait_recv()

            @pl.when(jnp.logical_not(can_recv))
            def _():
                fill()

        return arrive

    def left(slot):
        copy, can_send = sent[slot]

        @pl.when(can_send)
        def _():
            copy.wait_send()

    def setter(dst, src):
        def fill():
            dst[...] = src[...]

        return fill

    first, last = slice(0, 1), slice(ni - 1, ni)

    step[...] = jnp.zeros_like(step)

    def squares(oi, ox, oz):
        return fold(oi * oi + ox * ox + oz * oz)

    def pass_one(i, d1):
        here, limit = n[i + 1], b[i + 1]
        scaled = SIGMA * here
        di = clip(SIGMA * n[i + 2] - scaled, limit)
        dx = clip(ahead(scaled, 0) - scaled, limit)
        dz = clip(ahead(scaled, 1) - scaled, limit)
        dual[0, i] = di
        dual[1, i] = dx
        dual[2, i] = dz
        div = di - step[...]
        div = div + (dx - behind(dx, 0))
        div = div + (dz - behind(dz, 1))
        step[...] = di
        v[i + 1] = here + (2.0 * GAIN) * div
        return d1 + squares(di, dx, dz)

    zero = jnp.zeros((8, 128), jnp.float32)

    def pass_group(k, d1):
        for copy in chunk(k, GROUP):
            copy.wait()
        for at in range(GROUP):
            d1 = pass_one(GROUP * k + at, d1)
        return d1

    early = min(EARLY, groups)
    loads[0].wait()
    d1 = lax.fori_loop(0, early, pass_group, zero)
    for k in range(1, 10):
        loads[k].wait()
    zc_up[0:1], zc_up[1:2], zc_up[2:3], zc_up[3:4] = nx_first[last], nx_last[last], bx_first[last], bx_last[last]
    zc_down[0:1], zc_down[1:2] = nx_first[first], nx_last[first]
    xc_up[0:1], xc_up[1:2], xc_up[2:3], xc_up[3:4] = nx_last[first], nx_last[last], bx_last[first], bx_last[last]
    xc_down[0:1], xc_down[1:2] = nx_first[first], nx_first[last]
    pl.semaphore_wait(barrier, greeted)
    got_zc_prev = send(zc_up, zc_prev, "inl", True)
    got_zc_next = send(zc_down, zc_next, "inl", False)
    got_xc_prev = send(xc_up, xc_prev, "xln", True)
    got_xc_next = send(xc_down, xc_next, "xln", False)
    got_n_prev = send(n.at[top], n.at[0], "inl", True)
    got_n_next = send(n.at[1], n.at[end], "inl", False)
    got_b_prev = send(b.at[top], b.at[0], "inl", True)
    got_nx_prev = send(nx_last, nx_prev, "xln", True)
    got_nx_next = send(nx_first, nx_next, "xln", False)
    got_bx_prev = send(bx_last, bx_prev, "xln", True)

    def edge(here, limit, side):
        di = clip(SIGMA * (ahead(here, 0) - here), limit)
        dz = clip(SIGMA * (ahead(here, 1) - here), limit)
        return here + (2.0 * GAIN) * ((di - behind(di, 0)) + side + (dz - behind(dz, 1)))

    inward = clip(SIGMA * (nx_second[...] - nx_first[...]), bx_first[...])
    vx_first[...] = edge(nx_first[...], bx_first[...], inward)
    inward = clip(SIGMA * (nx_last[...] - nx_semi[...]), bx_semi[...])
    vx_last[...] = edge(nx_last[...], bx_last[...], -inward)

    d1 = lax.fori_loop(early, groups, pass_group, d1)
    tail.wait()
    tail_n.wait()
    here, limit = n[top], b[top]
    dx = clip(SIGMA * (ahead(here, 0) - here), limit)
    dz = clip(SIGMA * (ahead(here, 1) - here), limit)
    dual[1, ni - 1] = dx
    dual[2, ni - 1] = dz
    div = (dx - behind(dx, 0)) - clip(SIGMA * (here - n[top - 1]), b[top - 1])
    div = div + (dz - behind(dz, 1))
    v[top] = here + (2.0 * GAIN) * div
    d1 = d1 + fold(dx * dx + dz * dz)
    for i in range(groups * GROUP, ni - 1):
        d1 = pass_one(i, d1)

    def no_prev(dst):
        def fill():
            dst[...] = jnp.zeros_like(dst)

        return fill

    def no_next(dst, low, high):
        def fill():
            dst[0:1] = low
            dst[1:2] = high

        return fill

    def grow(dst, rows, amount):
        dst[rows] = dst[rows] + (2.0 * GAIN) * amount

    got_zc_prev(no_prev(zc_prev))
    got_zc_next(no_next(zc_next, nx_first[last], nx_last[last]))
    grow(vx_first, first, -clip(SIGMA * (nx_first[first] - zc_prev[0:1]), zc_prev[2:3]))
    grow(vx_last, first, -clip(SIGMA * (nx_last[first] - zc_prev[1:2]), zc_prev[3:4]))
    grow(vx_first, last, clip(SIGMA * (zc_next[0:1] - nx_first[last]), bx_first[last]))
    grow(vx_last, last, clip(SIGMA * (zc_next[1:2] - nx_last[last]), bx_last[last]))
    got_vx_prev = send(vx_last, vx_prev, "xln", True)
    got_vx_next = send(vx_first, vx_next, "xln", False)
    got_xc_prev(no_prev(xc_prev))
    got_xc_next(no_next(xc_next, nx_last[first], nx_last[last]))
    for k, (rows, layer) in enumerate(((first, 1), (last, top))):
        outer = clip(SIGMA * (xc_next[k : k + 1] - nx_last[rows]), bx_last[rows])
        grow(v.at[layer], slice(nx - 1, nx), outer)
        outer = clip(SIGMA * (nx_first[rows] - xc_prev[k : k + 1]), xc_prev[2 + k : 3 + k])
        grow(v.at[layer], slice(0, 1), -outer)
    v_up = len(sent)
    got_v_prev = send(v.at[top], v.at[0], "inl", True)
    v_down = len(sent)
    got_v_next = send(v.at[1], v.at[end], "inl", False)

    if one_stage(ni_dev, nx_dev):
        for di in (2, -2):
            beyond = my_i - di // 2
            knows = jnp.logical_and(beyond >= 0, beyond < ni_dev)

            @pl.when(jnp.logical_and(knows, jnp.logical_and(my_i + di >= 0, my_i + di < ni_dev)))
            def _():
                pl.semaphore_signal(
                    far_sem, inc=1, device_id={"inl": my_i + di}, device_id_type=pl.DeviceIdType.MESH
                )

    row = lax.broadcasted_iota(jnp.int32, (8, nz), 0)

    def inner_rows(value, lo, hi):
        parts = split(value, 0, 8)
        if lo == 0:
            parts[0] = jnp.where(row == 0, 0.0, parts[0])
        if hi == nx:
            parts[-1] = jnp.where(row == 7, 0.0, parts[-1])
        return jnp.concatenate(parts, axis=0)

    def below(value, tile):
        turned = [pltpu.roll(part, 7, 0) for part in split(value, 0, 8)]
        over = [value[-8:] if tile is None else pltpu.roll(tile, 7, 0)]
        return jnp.concatenate([jnp.where(row == 7, x, t) for x, t in zip(turned[1:] + over, turned)], axis=0)

    def above(value, tile):
        turned = [pltpu.roll(part, 1, 0) for part in split(value, 0, 8)]
        under = [jnp.zeros_like(value[:8]) if tile is None else pltpu.roll(tile, 1, 0)]
        return jnp.concatenate([jnp.where(row == 0, x, t) for x, t in zip(under + turned[:-1], turned)], axis=0)

    def pass_two(i, so_far, lo=0, hi=nx, fresh=True):
        p1, p2, d2 = so_far
        here, limit, base = v[i + 1, lo:hi], b[i + 1, lo:hi], n[i + 1, lo:hi]
        oi, ox, oz = dual[0, i, lo:hi], dual[1, i, lo:hi], dual[2, i, lo:hi]
        scaled = SIGMA * here
        di = clip(oi + (SIGMA * v[i + 2, lo:hi] - scaled), limit)
        dx = clip(ox + (below(scaled, SIGMA * v[i + 1, hi : hi + 8] if hi < nx else None) - scaled), limit)
        dz = clip(oz + (ahead(scaled, 1) - scaled), limit)
        if lo == 0:
            before = None
        elif fresh:
            before = v[i + 1, lo - 8 : lo]
            before = clip(dual[1, i, lo - 8 : lo] + SIGMA * (below(before, here[:8]) - before), b[i + 1, lo - 8 : lo])
        else:
            before = dual[1, i, lo - 8 : lo]
        dual[0, i, lo:hi] = di
        dual[1, i, lo:hi] = dx
        dual[2, i, lo:hi] = dz
        div = di - step[lo:hi]
        div = div + (dx - above(dx, before))
        div = div + (dz - behind(dz, 1))
        step[lo:hi] = di
        half = 0.5 * (here - base)
        change = GAIN * (div - half)
        out[i, lo:hi] = base + half + change
        inner = inner_rows(change, lo, hi)
        return (
            p1 + fold(half * half),
            p2 + fold(inner * inner),
            d2 + squares(di - oi, dx - ox, dz - oz),
        )

    def begin(lo, hi):
        step[lo:hi] = clip(
            dual[0, 1, lo:hi] + SIGMA * (v[3, lo:hi] - v[2, lo:hi]), b[2, lo:hi]
        )

    def middle(i, so_far):
        return pass_two(i, so_far, 8, nx - 8)

    def rim(i, so_far):
        return pass_two(i, pass_two(i, so_far, 0, 8), nx - 8, nx, False)

    begin(8, nx - 8)
    sums = stepped(2, ni - 2, middle, (zero,) * 3, MIDDLE)

    got_nx_prev(setter(nx_prev, nx_first))
    got_bx_prev(setter(bx_prev, bx_last))
    got_nx_next(setter(nx_next, nx_last))
    dx_last = clip(SIGMA * (nx_next[...] - nx_last[...]), bx_last[...])
    dxp = clip(SIGMA * (nx_first[...] - nx_prev[...]), bx_prev[...])
    dual[1, :, nx - 1, :] = dx_last
    dx_prev[...] = dxp
    dx_edge[...] = dx_last
    wx_last[...] = vx_last[...] + (2.0 * GAIN) * dx_last
    wx_first[...] = vx_first[...] - (2.0 * GAIN) * dxp
    v[2:top, nx - 1, :] = wx_last[1 : ni - 1]
    v[2:top, 0, :] = wx_first[1 : ni - 1]
    d1 = d1 + fold(dx_last * dx_last)

    begin(0, 8)
    begin(nx - 8, nx)
    sums = stepped(2, ni - 2, rim, sums, RIM)

    got_n_prev(setter(n.at[0], n.at[1]))
    got_b_prev(setter(b.at[0], b.at[1]))
    got_n_next(setter(n.at[end], n.at[top]))
    left(v_up)
    left(v_down)
    di_last = clip(SIGMA * (n[end] - n[top]), b[top])
    dip = clip(SIGMA * (n[1] - n[0]), b[0])
    dual[0, ni - 1] = di_last
    di_prev[...] = dip
    d1 = d1 + fold(di_last * di_last)
    v[top] = v[top] + (2.0 * GAIN) * di_last
    v[1] = v[1] - (2.0 * GAIN) * dip
    sums = pass_two(ni - 2, sums)
    step[...] = clip(dual[0, 0] + SIGMA * (v[2] - v[1]), b[1])
    sums = pass_two(1, sums)

    got_vx_prev(setter(vx_prev, wx_first))
    got_vx_next(setter(vx_next, wx_last))
    got_v_next(setter(v.at[end], v.at[top]))
    got_v_prev(setter(v.at[0], v.at[1]))
    v[end] = v[end] - (2.0 * GAIN) * dual[0, ni - 1]
    v[0] = v[0] + (2.0 * GAIN) * di_prev[...]
    step[...] = dual[0, ni - 2]
    sums = pass_two(ni - 1, sums)
    step[...] = clip(di_prev[...] + SIGMA * (v[1] - v[0]), b[0])
    p1, p2, d2 = pass_two(0, sums)

    was = dx_edge[...]
    dx_last = clip(
        was + SIGMA * (vx_next[...] - (2.0 * GAIN) * was - wx_last[...]), bx_last[...]
    )
    dual[1, :, nx - 1, :] = dx_last
    moved = dx_last - was
    d2 = d2 + fold(moved * moved)
    u_last = out[:, nx - 1, :] + GAIN * moved
    out[:, nx - 1, :] = u_last
    dxp = clip(
        dx_prev[...] + SIGMA * (wx_first[...] - (vx_prev[...] + (2.0 * GAIN) * dx_prev[...])), bx_prev[...]
    )
    u_first = out[:, 0, :] - GAIN * dxp
    out[:, 0, :] = u_first
    change = u_last - (nx_last[...] + 0.5 * (wx_last[...] - nx_last[...]))
    p2 = p2 + fold(change * change)
    change = u_first - (nx_first[...] + 0.5 * (wx_first[...] - nx_first[...]))
    p2 = p2 + fold(change * change)

    total = gather_lanes((p1, d1, p2, d2))
    if one_stage(ni_dev, nx_dev):
        far = 0
        for di in (3, -3):
            far = far + jnp.logical_and(my_i + di >= 0, my_i + di < ni_dev).astype(jnp.int32)
        if ni_dev > 3:
            @pl.when(far > 0)
            def _():
                pl.semaphore_wait(far_sem, 1)
    first = 0
    for stage, peers in enumerate(stages):
        mine[stage] = total
        for k, (di, dx) in enumerate(peers, first):
            pltpu.make_async_remote_copy(
                src_ref=mine.at[stage], dst_ref=others.at[k],
                send_sem=give_sem.at[stage], recv_sem=take_sem.at[stage],
                device_id=at(di, dx), device_id_type=pl.DeviceIdType.MESH,
            ).start()
        landed = others.at[pl.ds(first, len(peers))]
        if stage == 0:
            for slot in range(len(sent)):
                if slot not in (v_up, v_down):
                    left(slot)
        for sem in (give_sem, take_sem):
            pltpu.make_async_copy(landed, landed, sem.at[stage]).wait()
        rows = [total] + [others[k] for k in range(first, first + len(peers))]
        while len(rows) > 1:
            rows = [sum(rows[k + 1 : k + 2], rows[k]) for k in range(0, len(rows), 2)]
        total = rows[0]
        first += len(peers)
    norms[...] = jnp.sqrt(total[:, 0:2])


def put_out(out_held, dual_held, norms_held, out, dual, norms, sems):
    half = out.shape[0] // 2
    pairs = [(norms_held, norms)]
    for at in (0, half):
        part = pl.ds(at, half)
        pairs.append((out_held.at[part], out.at[part]))
        for axis in range(3):
            pairs.append((dual_held.at[axis, part], dual.at[axis, part]))
    copies = [pltpu.make_async_copy(src, dst, sems.at[k]) for k, (src, dst) in enumerate(pairs)]
    for copy in copies:
        copy.start()
    for copy in copies:
        copy.wait()


def per_device(noisy, bound):
    ni, nx, nz = noisy.shape
    ni_dev, nx_dev = lax.axis_size("inl"), lax.axis_size("xln")
    f32 = jnp.float32
    face = pltpu.VMEM((ni, nz), f32)
    slab = pltpu.VMEM((nx, nz), f32)
    dma = pltpu.SemaphoreType.DMA
    volume = 4 * ni * nx * nz
    stages = reduction(ni_dev, nx_dev)
    peers = sum(len(stage) for stage in stages)
    noisy = pltpu.with_memory_space_constraint(noisy, pltpu.HBM)
    bound = pltpu.with_memory_space_constraint(bound, pltpu.HBM)
    held = pl.pallas_call(
        functools.partial(kernel, ni_dev, nx_dev),
        out_shape=(
            pltpu.VMEM((ni, nx, nz), f32),
            pltpu.VMEM((3, ni, nx, nz), f32),
            pltpu.VMEM((2, 2), f32),
        ),
        in_specs=[pl.BlockSpec(memory_space=pltpu.HBM)] * 2,
        out_specs=(
            pl.BlockSpec(memory_space=pltpu.VMEM),
            pl.BlockSpec(memory_space=pltpu.VMEM),
            pl.BlockSpec(memory_space=pltpu.VMEM),
        ),
        scratch_shapes=[
            pltpu.VMEM((ni + 2, nx, nz), f32),
            pltpu.VMEM((ni + 1, nx, nz), f32),
            pltpu.VMEM((ni + 2, nx, nz), f32),
            slab,
            *([face] * 18),
            slab,
            *([pltpu.VMEM((4, nz), f32), pltpu.VMEM((2, nz), f32)] * 4),
            pltpu.VMEM((len(stages), 2, 128), f32),
            pltpu.VMEM((peers, 2, 128), f32),
            dma((10,)), dma((2, (ni - 1) // GROUP + 1)), dma((14,)), dma((14,)), dma((len(stages),)), dma((len(stages),)),
            pltpu.SemaphoreType.REGULAR,
        ],
        compiler_params=pltpu.CompilerParams(
            collective_id=0, has_side_effects=True, vmem_limit_bytes=24 * 1024 * 1024
        ),
        cost_estimate=pl.CostEstimate(
            flops=80 * ni * nx * nz, bytes_accessed=6 * volume, transcendentals=0
        ),
        name="denoise",
    )(noisy, bound)
    in_vmem = pl.BlockSpec(memory_space=pltpu.VMEM)
    in_hbm = pl.BlockSpec(memory_space=pltpu.HBM)
    return pl.pallas_call(
        put_out,
        out_shape=(
            jax.ShapeDtypeStruct((ni, nx, nz), f32),
            jax.ShapeDtypeStruct((3, ni, nx, nz), f32),
            jax.ShapeDtypeStruct((2, 2), f32),
        ),
        in_specs=[in_vmem] * 3,
        out_specs=(in_hbm,) * 3,
        scratch_shapes=[dma((9,))],
        compiler_params=pltpu.CompilerParams(vmem_limit_bytes=1024 * 1024),
        cost_estimate=pl.CostEstimate(flops=0, bytes_accessed=4 * volume, transcendentals=0),
        name="put_out",
    )(*held)


def solution(mesh):
    in_specs = (P("inl", "xln", None), P("inl", "xln", None))
    out_specs = (P("inl", "xln", None), P(None, "inl", "xln", None), P())
    return jax.shard_map(
        per_device, mesh=mesh, in_specs=in_specs, out_specs=out_specs, check_vma=False
    )
```
